256 devices in a mesh: rows: 32 (over y, x, core), feat: 8 (over z).
Axes of the slice: x: 4, y: 4, z: 8, core: 2. Of those that a mesh axis runs over, the one named last changes fastest.
Arguments:
- features: bfloat16 [32768, 2048], P('rows', 'feat'), may hold values from -6 to 6
- grad_out: bfloat16 [32768, 2048], P('rows', 'feat'), may hold values from -6 to 6
- eigvecs: float32 [2048, 2048], P('feat', 'rows'), may hold values from -1 to 1, as said below
- eigvals: float32 [2048], replicated, may hold values from 0.1 to 1, as said below
- whiten: bfloat16 [2048, 2048], P(None, 'feat'), may hold values from -0.125 to 0.125
Outputs:
- grad_in: bfloat16 [32768, 2048], P('rows', 'feat')
The draws below stay inside these ranges and needn't reach their ends.
Inputs may be any that keep to these rules, and one draw needn't show every extreme that they name: `eigvecs`: the columns are orthonormal. `eigvals`: any two entries differ by at least 0.45 / 2048.
All inputs are finite; a program needn't handle non-finite values.
Results may differ from the reference program's by a relative error of at most 0.0074.
Values may be sent and summed in bfloat16 or wider, within the bound.
No kernel may reach another device: no remote copies, remote signals or barrier semaphores. Data moves between devices by JAX's collectives and lax.ppermute only.
A program may use at most 128 MiB of HBM per device.

```python
import jax
import jax.numpy as jnp
from jax import lax

D = 2048
TOKENS = 32768


def draw_eigvecs(key, part):
    normal_mat = jax.random.normal(key, (D, D), jnp.float32)
    ortho, upper = jnp.linalg.qr(normal_mat)
    return ortho


def draw_eigvals(key, part):
    ranking = jax.random.permutation(jax.random.fold_in(key, 1), D)
    jitter = jax.random.uniform(jax.random.fold_in(key, 2), (D,), jnp.float32)
    return 0.1 + 0.9 * (ranking.astype(jnp.float32) + 0.25 + 0.5 * jitter) / D


def block_levels(own_key, extent, shards, low, top_value):
    loudness, own = 1.0, jax.random.fold_in(own_key, 6)
    for dim, parts in shards:
        heights = jnp.exp(jax.random.uniform(jax.random.fold_in(own, dim), (parts,), jnp.float32, low / len(shards), top_value / len(shards)))
        loudness = loudness * jnp.repeat(heights, extent[dim] // parts).reshape([-1 if axis == dim else 1 for axis in range(len(extent))])
    return loudness


def gaussian(own_key, extent, width, bound, split=(), held_as=jnp.bfloat16):
    entries = width * jax.random.normal(own_key, extent, jnp.float32)
    if split:
        entries = entries * block_levels(own_key, extent, split, -0.22, 0.18)
    return jnp.clip(entries, -bound, bound).astype(held_as)


def setup_inputs(seed: int = 0) -> dict:
    keys = jax.random.split(jax.random.key(seed), 6)
    return {
        "features": gaussian(keys[0], (TOKENS, D), 1.0, 6.0, ((0, 32), (1, 8))),
        "grad_out": gaussian(keys[1], (TOKENS, D), 1.0, 6.0, ((0, 32), (1, 8))),
        "eigvecs": draw_eigvecs(jax.random.fold_in(keys[5], 71), 0),
        "eigvals": draw_eigvals(jax.random.fold_in(keys[5], 71), 0),
        "whiten": gaussian(keys[4], (D, D), D ** -0.5, 0.125, ((1, 8),)),
    }


def divided(lam_row, lam_col, first_col):
    on_diag = jnp.arange(lam_row.shape[0], dtype=jnp.int32)[:, None] == (first_col + jnp.arange(lam_col.shape[0], dtype=jnp.int32))[None, :]
    root_row = lam_row ** (-0.5)
    root_col = lam_col ** (-0.5)
    gaps_lam = lam_row[:, None] - lam_col[None, :]
    safe_gap = jnp.where(on_diag, jnp.ones_like(gaps_lam), gaps_lam)
    off_diag = (root_row[:, None] - root_col[None, :]) / safe_gap
    diag_vals = -0.5 * lam_row[:, None] ** (-1.5) + jnp.zeros_like(gaps_lam)
    return jnp.where(on_diag, diag_vals, off_diag)

def reference(features, grad_out, eigvecs, eigvals, whiten):
    highest = lax.Precision.HIGHEST
    row_count = features.shape[0]
    col_mean = jnp.sum(features.astype(jnp.float32), axis=0) / row_count
    grad_mean = jnp.sum(grad_out.astype(jnp.float32), axis=0) / row_count
    cross_prod = jnp.dot(features.T.astype(jnp.float32), grad_out.astype(jnp.float32), preferred_element_type=jnp.float32) - row_count * jnp.outer(col_mean, grad_mean)
    sym_gram = 0.5 * (cross_prod + cross_prod.T)
    rotated = jnp.dot(eigvecs.T, jnp.dot(sym_gram, eigvecs, precision=highest), precision=highest)
    kernel = divided(eigvals, eigvals, 0)
    sens = jnp.dot(jnp.dot(eigvecs, kernel * rotated, precision=highest), eigvecs.T, precision=highest)
    sens_scaled = (2.0 / row_count * sens).astype(jnp.bfloat16)
    shifted = (grad_out.astype(jnp.float32) - grad_mean).astype(jnp.bfloat16)
    centered = (features.astype(jnp.float32) - col_mean).astype(jnp.bfloat16)
    grad_in = jnp.dot(shifted.astype(jnp.float32), whiten.astype(jnp.float32), preferred_element_type=jnp.float32) + jnp.dot(centered.astype(jnp.float32), sens_scaled.T.astype(jnp.float32), preferred_element_type=jnp.float32)
    return grad_in.astype(jnp.bfloat16)
```

```python
import jax
import jax.numpy as jnp
from jax import lax
from jax.sharding import PartitionSpec as P

F32 = jnp.float32
BF16 = jnp.bfloat16
CHUNKS = 2


def copy_for_each(shard, axis):
    copies = jnp.broadcast_to(shard, (lax.axis_size(axis), *shard.shape))
    return lax.all_to_all(copies, axis, split_axis=0, concat_axis=0, tiled=True)


def exchange(parts, axis):
    return lax.all_to_all(parts, axis, split_axis=0, concat_axis=0, tiled=True)


def contract_first(a, b):
    return lax.dot_general(a, b, (((0,), (0,)), ((), ())), preferred_element_type=F32)


def three_parts(x):
    a = lax.reduce_precision(x, 8, 7)
    b = lax.reduce_precision(x - a, 8, 7)
    c = x - a - b
    return [part.astype(BF16) for part in (a, b, c)]


def divided(lam_row, lam_col, first_col):
    on_diag = (
        jnp.arange(lam_row.shape[0], dtype=jnp.int32)[:, None]
        == (first_col + jnp.arange(lam_col.shape[0], dtype=jnp.int32))[None, :]
    )
    root_row = lam_row ** (-0.5)
    root_col = lam_col ** (-0.5)
    gaps_lam = lam_row[:, None] - lam_col[None, :]
    safe_gap = jnp.where(on_diag, jnp.ones_like(gaps_lam), gaps_lam)
    off_diag = (root_row[:, None] - root_col[None, :]) / safe_gap
    diag_vals = -0.5 * lam_row[:, None] ** (-1.5) + jnp.zeros_like(gaps_lam)
    return jnp.where(on_diag, diag_vals, off_diag)


def local(features, grad_out, eigvecs, eigvals, whiten):
    n, width = features.shape
    groups, planes = lax.axis_size("rows"), lax.axis_size("feat")
    total = n * groups
    dim = width * planes
    narrow = eigvecs.shape[1]
    half = planes // 2
    r, f = lax.axis_index("rows"), lax.axis_index("feat")
    way = jnp.where(r % 2 == 0, -1, 1)
    ring = [
        (a * planes + b, a * planes + (b + (1 if a % 2 == 0 else -1)) % planes)
        for a in range(groups)
        for b in range(planes)
    ]

    step = n // CHUNKS
    cut = lambda a, k: a[k * step : (k + 1) * step]
    own = [jnp.concatenate([cut(features, k), cut(grad_out, k)]) for k in range(CHUNKS)]
    blocks = [[jnp.concatenate([cut(grad_out, k), cut(features, k)]) for k in range(CHUNKS)]]
    for _ in range(planes - 1):
        blocks.append([lax.ppermute(b, ("rows", "feat"), ring) for b in blocks[-1]])

    sums = jnp.stack([jnp.sum(a, axis=0, dtype=F32) for a in (features, grad_out)])
    means = jnp.sum(copy_for_each(sums, "rows"), axis=0) / total
    packed = [p.reshape(-1, narrow) for p in three_parts(means)]
    shared = copy_for_each(jnp.concatenate([eigvecs.astype(BF16), *packed]), "feat")
    basis_r = shared[:, :width].reshape(dim, narrow)
    all_means = jnp.sum(
        shared[:, width:].astype(F32).reshape(planes, 3, 2, width), axis=1
    )
    basis_t = lax.all_gather(basis_r.T, "rows", axis=0, tiled=True)

    def outer(a, b):
        return a[:, None] * b[None, :]

    parts = []
    for h in range(half + 1):
        there = lax.dynamic_index_in_dim(all_means, (f + way * h) % planes, 0, False)
        if h == 0:
            raw = contract_first(features, grad_out)
            raw -= outer(sums[0], means[1]) + outer(means[0], sums[1] - n * means[1])
        else:
            raw = sum(contract_first(a, b) for a, b in zip(own, blocks[h]))
            sum_g = sum(jnp.sum(b[:step], axis=0, dtype=F32) for b in blocks[h])
            sum_x = sum(jnp.sum(b[step:], axis=0, dtype=F32) for b in blocks[h])
            raw -= outer(sums[0], there[1]) + outer(sums[1], there[0])
            raw -= outer(means[0], sum_g - n * there[1]) + outer(means[1], sum_x - n * there[0])
            if h == half:
                raw = 0.5 * raw
        parts.append(raw.astype(BF16))
    mixed = jnp.concatenate(parts, axis=1)

    got = exchange(mixed.reshape(groups, width // groups, -1), "rows").astype(F32)
    got = jnp.sum(got.reshape(groups // 2, 2, width // groups, -1), axis=0)
    piece = lambda c, h: got[c, :, h * width : (h + 1) * width]
    pair = [piece(0, 0) + piece(1, 0)]
    pair += [piece(1, h) for h in range(1, half)]
    pair += [piece(0, half) + piece(1, half)]
    pair += [piece(0, h) for h in range(half - 1, 0, -1)]
    gram = copy_for_each(jnp.concatenate(pair, axis=1).astype(BF16), "rows")
    gram = gram.reshape(width, dim)

    twice = jnp.concatenate([basis_r, basis_r])
    turned = lax.dynamic_slice_in_dim(twice, f * width, dim)
    right = jnp.dot(gram, turned, preferred_element_type=F32).astype(BF16)
    right = copy_for_each(right, "feat").reshape(dim, narrow)
    rot = jnp.dot(basis_t, right, preferred_element_type=F32)
    back = exchange(rot.astype(BF16).reshape(groups, narrow, narrow), "rows")
    rot = rot + jnp.swapaxes(back, 1, 2).reshape(dim, narrow).astype(F32)
    first_col = r * narrow
    lam_col = lax.dynamic_slice_in_dim(eigvals, first_col, narrow)
    scaled = divided(eigvals, lam_col, first_col) * rot

    high = lax.reduce_precision(scaled, 8, 7)
    both = jnp.concatenate([high.astype(BF16), (scaled - high).astype(BF16)], axis=1)
    basis_f = lax.dynamic_slice_in_dim(basis_t, f * width, width, axis=1)
    undone = contract_first(both, basis_f)
    undone = (undone[:narrow] + undone[narrow:]).astype(BF16)
    undone = copy_for_each(undone, "rows").reshape(dim, width)
    sens = contract_first(basis_t, undone)
    sens_scaled = (sens * (1.0 / total)).astype(BF16)

    shifted = jnp.zeros((n, dim), BF16)
    centered = jnp.zeros((n, dim), BF16)
    for h in range(planes):
        g = (f + way * h) % planes
        there = lax.dynamic_index_in_dim(all_means, g, 0, False)
        for k, b in enumerate(blocks[h]):
            at = (k * step, g * width)
            shifted = lax.dynamic_update_slice(
                shifted, (b[:step].astype(F32) - there[1]).astype(BF16), at
            )
            centered = lax.dynamic_update_slice(
                centered, (b[step:].astype(F32) - there[0]).astype(BF16), at
            )
    grad_in = jnp.dot(shifted, whiten, preferred_element_type=F32)
    grad_in = grad_in + jnp.dot(centered, sens_scaled, preferred_element_type=F32)
    return grad_in.astype(BF16)


def solution(mesh):
    in_specs = (P("rows", "feat"), P("rows", "feat"), P("feat", "rows"), P(), P(None, "feat"))
    out_specs = P("rows", "feat")
    return jax.shard_map(local, mesh=mesh, in_specs=in_specs, out_specs=out_specs, check_vma=False)
```

```python
import jax
import jax.numpy as jnp
from jax import lax
from jax.sharding import PartitionSpec as P


F32 = jnp.float32
BF16 = jnp.bfloat16


def copy_for_each(shard, axis):
    copies = jnp.broadcast_to(shard, (lax.axis_size(axis), *shard.shape))
    return lax.all_to_all(copies, axis, split_axis=0, concat_axis=0, tiled=True)


def exchange(parts, axis):
    return lax.all_to_all(parts, axis, split_axis=0, concat_axis=0, tiled=True)


def contract_first(a, b):
    return lax.dot_general(a, b, (((0,), (0,)), ((), ())), preferred_element_type=F32)


def contract_last(a, b):
    return lax.dot_general(a, b, (((1,), (1,)), ((), ())), preferred_element_type=F32)


def three_parts(x):
    a = lax.reduce_precision(x, 8, 7)
    b = lax.reduce_precision(x - a, 8, 7)
    c = x - a - b
    return [part.astype(BF16) for part in (a, b, c)]


def divided(lam_row, lam_col, first_col):
    on_diag = (
        jnp.arange(lam_row.shape[0], dtype=jnp.int32)[:, None]
        == (first_col + jnp.arange(lam_col.shape[0], dtype=jnp.int32))[None, :]
    )
    root_row = lam_row ** (-0.5)
    root_col = lam_col ** (-0.5)
    gaps_lam = lam_row[:, None] - lam_col[None, :]
    safe_gap = jnp.where(on_diag, jnp.ones_like(gaps_lam), gaps_lam)
    off_diag = (root_row[:, None] - root_col[None, :]) / safe_gap
    diag_vals = -0.5 * lam_row[:, None] ** (-1.5) + jnp.zeros_like(gaps_lam)
    return jnp.where(on_diag, diag_vals, off_diag)


def local(features, grad_out, eigvecs, eigvals, whiten):
    n, width = features.shape
    groups, planes = lax.axis_size("rows"), lax.axis_size("feat")
    total = n * groups
    dim = width * planes
    narrow = eigvecs.shape[1]
    half = planes // 2
    r, f = lax.axis_index("rows"), lax.axis_index("feat")
    way = jnp.where(r % 2 == 0, -1, 1)
    ring = [
        (a * planes + b, a * planes + (b + (1 if a % 2 == 0 else -1)) % planes)
        for a in range(groups)
        for b in range(planes)
    ]

    blocks = [(grad_out, features)]
    for _ in range(1, planes):
        blocks.append(tuple(lax.ppermute(b, ("rows", "feat"), ring) for b in blocks[-1]))

    sums = jnp.stack([jnp.sum(a, axis=0, dtype=F32) for a in (features, grad_out)])
    means = jnp.sum(copy_for_each(sums, "rows"), axis=0) / total
    shared = jnp.concatenate([eigvecs.astype(BF16).T, *three_parts(means)])
    shared = copy_for_each(shared, "feat")
    basis_rt = jnp.swapaxes(shared[:, :narrow], 0, 1).reshape(narrow, dim)
    all_means = jnp.sum(
        shared[:, narrow:].astype(F32).reshape(planes, 3, 2, width), axis=1
    )
    basis_t = lax.all_gather(basis_rt, "rows", axis=0, tiled=True)

    def outer(a, b):
        return a[:, None] * b[None, :]

    parts = []
    for h in range(half + 1):
        there = lax.dynamic_index_in_dim(all_means, (f + way * h) % planes, 0, False)
        if h == 0:
            raw = contract_first(features, grad_out)
            raw -= outer(sums[0], means[1]) + outer(means[0], sums[1] - n * means[1])
        else:
            raw = contract_first(features, blocks[h][0]) + contract_first(grad_out, blocks[h][1])
            sum_g, sum_x = (jnp.sum(b, axis=0, dtype=F32) for b in blocks[h])
            raw -= outer(sums[0], there[1]) + outer(sums[1], there[0])
            raw -= outer(means[0], sum_g - n * there[1]) + outer(means[1], sum_x - n * there[0])
            if h == half:
                raw = 0.5 * raw
        parts.append(raw.astype(BF16))
    mixed = jnp.concatenate(parts, axis=1)

    got = exchange(mixed.reshape(groups, width // groups, -1), "rows").astype(F32)
    got = jnp.sum(got.reshape(groups // 2, 2, width // groups, -1), axis=0)
    piece = lambda c, h: got[c, :, h * width : (h + 1) * width]
    pair = [piece(0, 0) + piece(1, 0)]
    pair += [piece(1, h) for h in range(1, half)]
    pair += [piece(0, half) + piece(1, half)]
    pair += [piece(0, h) for h in range(half - 1, 0, -1)]
    gram = copy_for_each(jnp.concatenate(pair, axis=1).astype(BF16), "rows")
    gram = gram.reshape(width, dim)

    twice = jnp.concatenate([basis_rt, basis_rt], axis=1)
    turned = lax.dynamic_slice_in_dim(twice, f * width, dim, axis=1)
    right = contract_last(gram, turned).astype(BF16)
    right = copy_for_each(right, "feat").reshape(dim, narrow)
    rot = jnp.dot(basis_t, right, preferred_element_type=F32)
    back = exchange(rot.astype(BF16).reshape(groups, narrow, narrow), "rows")
    rot = rot + jnp.swapaxes(back, 1, 2).reshape(dim, narrow).astype(F32)
    first_col = r * narrow
    lam_col = lax.dynamic_slice_in_dim(eigvals, first_col, narrow)
    scaled = divided(eigvals, lam_col, first_col) * rot

    high = lax.reduce_precision(scaled, 8, 7)
    both = jnp.concatenate([high.astype(BF16), (scaled - high).astype(BF16)], axis=1)
    basis_f = lax.dynamic_slice_in_dim(basis_t, f * width, width, axis=1)
    undone = contract_first(both, basis_f)
    undone = (undone[:narrow] + undone[narrow:]).astype(BF16)
    undone = copy_for_each(undone, "rows").reshape(dim, width)
    sens = contract_first(basis_t, undone)
    sens_scaled = lax.optimization_barrier((sens * (1.0 / total)).astype(BF16))

    grad_in = jnp.zeros((n, width), F32)
    centered = jnp.zeros((n, dim), BF16)
    for h in range(planes):
        g = (f + way * h) % planes
        there = lax.dynamic_index_in_dim(all_means, g, 0, False)
        grads, inputs = blocks[h]
        at = (0, g * width)
        shifted = (grads.astype(F32) - there[1]).astype(BF16)
        mine = lax.dynamic_slice_in_dim(whiten, g * width, width)
        grad_in += jnp.dot(shifted, mine, preferred_element_type=F32)
        centered = lax.dynamic_update_slice(
            centered, (inputs.astype(F32) - there[0]).astype(BF16), at
        )
    grad_in += jnp.dot(centered, sens_scaled, preferred_element_type=F32)
    return grad_in.astype(BF16)


def solution(mesh):
    in_specs = (P("rows", "feat"), P("rows", "feat"), P("feat", "rows"), P(), P(None, "feat"))
    out_specs = P("rows", "feat")
    return jax.shard_map(local, mesh=mesh, in_specs=in_specs, out_specs=out_specs, check_vma=False)
```

```python
import jax
import jax.numpy as jnp
from jax import lax
from jax.sharding import PartitionSpec as P


F32 = jnp.float32
BF16 = jnp.bfloat16


def copy_for_each(shard, axis):
    copies = jnp.broadcast_to(shard, (lax.axis_size(axis), *shard.shape))
    return lax.all_to_all(copies, axis, split_axis=0, concat_axis=0, tiled=True)


def exchange(parts, axis):
    return lax.all_to_all(parts, axis, split_axis=0, concat_axis=0, tiled=True)


def contract_first(a, b):
    return lax.dot_general(a, b, (((0,), (0,)), ((), ())), preferred_element_type=F32)


def contract_last(a, b):
    return lax.dot_general(a, b, (((1,), (1,)), ((), ())), preferred_element_type=F32)


def three_parts(x):
    a = lax.reduce_precision(x, 8, 7)
    b = lax.reduce_precision(x - a, 8, 7)
    c = x - a - b
    return [part.astype(BF16) for part in (a, b, c)]


def divided(lam_row, lam_col, first_col):
    on_diag = (
        jnp.arange(lam_row.shape[0], dtype=jnp.int32)[:, None]
        == (first_col + jnp.arange(lam_col.shape[0], dtype=jnp.int32))[None, :]
    )
    root_row = lam_row ** (-0.5)
    root_col = lam_col ** (-0.5)
    gaps_lam = lam_row[:, None] - lam_col[None, :]
    safe_gap = jnp.where(on_diag, jnp.ones_like(gaps_lam), gaps_lam)
    off_diag = (root_row[:, None] - root_col[None, :]) / safe_gap
    diag_vals = -0.5 * lam_row[:, None] ** (-1.5) + jnp.zeros_like(gaps_lam)
    return jnp.where(on_diag, diag_vals, off_diag)


def local(features, grad_out, eigvecs, eigvals, whiten):
    n, width = features.shape
    groups, planes = lax.axis_size("rows"), lax.axis_size("feat")
    total = n * groups
    dim = width * planes
    narrow = eigvecs.shape[1]
    half = planes // 2
    r, f = lax.axis_index("rows"), lax.axis_index("feat")
    way = jnp.where(r % 2 == 0, -1, 1)
    ring = [
        (a * planes + b, a * planes + (b + (1 if a % 2 == 0 else -1)) % planes)
        for a in range(groups)
        for b in range(planes)
    ]

    blocks = [(grad_out, features)]
    for _ in range(1, planes):
        blocks.append(tuple(lax.ppermute(b, ("rows", "feat"), ring) for b in blocks[-1]))

    sums = jnp.stack([jnp.sum(a, axis=0, dtype=F32) for a in (features, grad_out)])
    means = jnp.sum(copy_for_each(sums, "rows"), axis=0) / total
    two_on = [
        (a * planes + b, a * planes + (b + (2 if a % 2 == 0 else -2)) % planes)
        for a in range(groups)
        for b in range(planes)
    ]
    packed = jnp.concatenate(three_parts(means))
    told = [packed, lax.ppermute(packed, ("rows", "feat"), ring)]
    told.append(lax.ppermute(packed, ("rows", "feat"), two_on))
    for _ in range(3, planes):
        told.append(lax.ppermute(told[-1], ("rows", "feat"), ring))
    told = [jnp.sum(t.astype(F32).reshape(3, 2, width), axis=0) for t in told]
    basis_rt = copy_for_each(eigvecs.astype(BF16).T, "feat")
    basis_rt = jnp.swapaxes(basis_rt, 0, 1).reshape(narrow, dim)
    basis_t = lax.all_gather(basis_rt, "rows", axis=0, tiled=True)

    def outer(a, b):
        return a[:, None] * b[None, :]

    parts = []
    for h in range(half + 1):
        there = told[h]
        grads, inputs = blocks[h]
        raw = contract_first(features, grads)
        if h == 0:
            raw -= outer(sums[0], means[1]) + outer(means[0], sums[1] - n * means[1])
        else:
            also = contract_first(grad_out, inputs)
            sum_g, sum_x = (jnp.sum(b, axis=0, dtype=F32) for b in blocks[h])
            raw += also
            raw -= outer(sums[0], there[1]) + outer(sums[1], there[0])
            raw -= outer(means[0], sum_g - n * there[1])
            raw -= outer(means[1], sum_x - n * there[0])
        if h == half:
            raw = 0.5 * raw
        parts.append(raw.astype(BF16))
    mixed = jnp.concatenate(parts, axis=1)

    got = exchange(mixed.reshape(groups, width // groups, -1), "rows").astype(F32)
    got = jnp.sum(got.reshape(groups // 2, 2, width // groups, -1), axis=0)
    piece = lambda c, h: got[c, :, h * width : (h + 1) * width]
    pair = [piece(0, 0) + piece(1, 0)]
    pair += [piece(1, h) for h in range(1, half)]
    pair += [piece(0, half) + piece(1, half)]
    pair += [piece(0, h) for h in range(half - 1, 0, -1)]
    gram = copy_for_each(jnp.concatenate(pair, axis=1).astype(BF16), "rows")
    gram = gram.reshape(width, dim)

    twice = jnp.concatenate([basis_rt, basis_rt], axis=1)
    turned = lax.dynamic_slice_in_dim(twice, f * width, dim, axis=1)
    right = contract_last(gram, turned).astype(BF16)
    right = copy_for_each(right, "feat").reshape(dim, narrow)
    rot = jnp.dot(basis_t, right, preferred_element_type=F32)
    back = exchange(rot.astype(BF16).reshape(groups, narrow, narrow), "rows")
    rot = rot + jnp.swapaxes(back, 1, 2).reshape(dim, narrow).astype(F32)
    first_col = r * narrow
    lam_col = lax.dynamic_slice_in_dim(eigvals, first_col, narrow)
    scaled = divided(eigvals, lam_col, first_col) * rot

    high = lax.reduce_precision(scaled, 8, 7)
    both = jnp.concatenate([high.astype(BF16), (scaled - high).astype(BF16)], axis=1)
    basis_f = lax.dynamic_slice_in_dim(basis_t, f * width, width, axis=1)
    undone = contract_first(both, basis_f)
    undone = (undone[:narrow] + undone[narrow:]).astype(BF16)
    undone = copy_for_each(undone, "rows").reshape(dim, width)
    grad_in = jnp.zeros((n, width), F32)
    centered = jnp.zeros((n, dim), BF16)
    for h in range(planes):
        g = (f + way * h) % planes
        there = told[h]
        grads, inputs = blocks[h]
        at = (0, g * width)
        shifted = (grads.astype(F32) - there[1]).astype(BF16)
        mine = lax.dynamic_slice_in_dim(whiten, g * width, width)
        grad_in += jnp.dot(shifted, mine, preferred_element_type=F32)
        centered = lax.dynamic_update_slice(
            centered, (inputs.astype(F32) - there[0]).astype(BF16), at
        )
    part = n // 2
    out = []
    for k in range(2):
        rows = slice(k * part, (k + 1) * part)
        turned = contract_last(centered[rows], basis_t).astype(BF16)
        last = jnp.dot(lax.optimization_barrier(turned), undone, preferred_element_type=F32)
        out.append((grad_in[rows] + last * (1.0 / total)).astype(BF16))
    return jnp.concatenate(out)


def solution(mesh):
    in_specs = (P("rows", "feat"), P("rows", "feat"), P("feat", "rows"), P(), P(None, "feat"))
    out_specs = P("rows", "feat")
    return jax.shard_map(local, mesh=mesh, in_specs=in_specs, out_specs=out_specs, check_vma=False)
```

```python
import jax
import jax.numpy as jnp
from jax import lax
from jax.experimental import pallas as pl
from jax.experimental.pallas import tpu as pltpu
from jax.sharding import PartitionSpec as P


F32 = jnp.float32
BF16 = jnp.bfloat16
VMEM = pl.BlockSpec(memory_space=pltpu.VMEM)
LIMIT = 40 * 1024 * 1024


def copy_for_each(shard, axis):
    copies = jnp.broadcast_to(shard, (lax.axis_size(axis), *shard.shape))
    return lax.all_to_all(copies, axis, split_axis=0, concat_axis=0, tiled=True)


def exchange(parts, axis):
    return lax.all_to_all(parts, axis, split_axis=0, concat_axis=0, tiled=True)


def contract_last(a, b):
    return lax.dot_general(a, b, (((1,), (1,)), ((), ())), preferred_element_type=F32)


def product(a, b):
    return jnp.dot(a, b, preferred_element_type=F32)


def three_parts(x):
    a = lax.reduce_precision(x, 8, 7)
    b = lax.reduce_precision(x - a, 8, 7)
    c = x - a - b
    return [part.astype(BF16) for part in (a, b, c)]


def divided(lam_row, lam_col, first_row):
    on_diag = (
        (first_row + jnp.arange(lam_row.shape[0], dtype=jnp.int32))[:, None]
        == jnp.arange(lam_col.shape[0], dtype=jnp.int32)[None, :]
    )
    root_row = lam_row ** (-0.5)
    root_col = lam_col ** (-0.5)
    gaps_lam = lam_row[:, None] - lam_col[None, :]
    safe_gap = jnp.where(on_diag, jnp.ones_like(gaps_lam), gaps_lam)
    off_diag = (root_row[:, None] - root_col[None, :]) / safe_gap
    diag_vals = -0.5 * lam_row[:, None] ** (-1.5) + jnp.zeros_like(gaps_lam)
    return jnp.where(on_diag, diag_vals, off_diag)


def cost(flops, nbytes):
    return pl.CostEstimate(flops=flops, bytes_accessed=nbytes, transcendentals=0)


def params():
    return pltpu.CompilerParams(vmem_limit_bytes=LIMIT)


def gram_body(hops, half, n, own_ref, mean_ref, told_ref, *refs):
    out_ref = refs[-1]
    xt, gt = own_ref[:, :n], own_ref[:, n:]
    sum_x = jnp.sum(xt.astype(F32), axis=1, keepdims=True)
    sum_g = jnp.sum(gt.astype(F32), axis=1, keepdims=True)
    mean_x, mean_g = mean_ref[:, 0:1], mean_ref[:, 1:2]
    width = xt.shape[0]
    for i, h in enumerate(hops):
        grads, inputs = refs[2 * i][...], refs[2 * i + 1][...]
        there_x, there_g = told_ref[2 * i : 2 * i + 1, :], told_ref[2 * i + 1 : 2 * i + 2, :]
        left_g = jnp.sum(grads.astype(F32), axis=0, keepdims=True) - n * there_g
        value = product(xt, grads) - (sum_x * there_g + mean_x * left_g)
        if h > 0:
            left_x = jnp.sum(inputs.astype(F32), axis=0, keepdims=True) - n * there_x
            value += product(gt, inputs) - (sum_g * there_x + mean_g * left_x)
        if h == half:
            value = 0.5 * value
        out_ref[:, i * width : (i + 1) * width] = value.astype(BF16)


def gram_first(own, mean_cols, told, blocks, half):
    width, n = own.shape[0], own.shape[1] // 2
    flat = [b for pair in blocks for b in pair]
    return pl.pallas_call(
        lambda *refs: gram_body(range(half), half, n, *refs),
        out_shape=jax.ShapeDtypeStruct((width, (half + 1) * width), BF16),
        grid=(1,),
        in_specs=[VMEM] * (3 + len(flat)),
        out_specs=pl.BlockSpec((width, half * width), lambda i: (0, 0)),
        compiler_params=params(),
        cost_estimate=cost(4 * half * n * width * width, 2 * n * width * 2 * (half + 1)),
        name="gram_first",
    )(own, mean_cols, told, *flat)


def gram_last(partial, own, mean_cols, told, block, half):
    width, n = own.shape[0], own.shape[1] // 2

    def body(partial_ref, *refs):
        gram_body((half,), half, n, *refs)

    return pl.pallas_call(
        body,
        out_shape=jax.ShapeDtypeStruct(partial.shape, BF16),
        grid=(1,),
        in_specs=[pl.BlockSpec(memory_space=pl.ANY)] + [VMEM] * 5,
        out_specs=pl.BlockSpec((width, width), lambda i: (0, half)),
        input_output_aliases={0: 0},
        compiler_params=params(),
        cost_estimate=cost(4 * n * width * width, 8 * n * width),
        name="gram_last",
    )(partial, own, mean_cols, told, *block)


def gathered_sum(got, width, half):
    groups, few, _ = got.shape

    def body(got_ref, out_ref):
        def add(i, sums):
            return sums[0] + got_ref[2 * i].astype(F32), sums[1] + got_ref[2 * i + 1].astype(F32)

        zero = jnp.zeros(got_ref.shape[1:], F32)
        down, up = lax.fori_loop(0, groups // 2, add, (zero, zero))
        piece = lambda a, h: a[:, h * width : (h + 1) * width]
        pair = [piece(down, 0) + piece(up, 0)]
        pair += [piece(up, h) for h in range(1, half)]
        pair += [piece(down, half) + piece(up, half)]
        pair += [piece(down, h) for h in range(half - 1, 0, -1)]
        value = jnp.concatenate(pair, axis=1).astype(BF16)

        def store(i, carry):
            out_ref[i] = value
            return carry

        lax.fori_loop(0, groups, store, 0)

    return pl.pallas_call(
        body,
        out_shape=jax.ShapeDtypeStruct((groups, few, 2 * half * width), BF16),
        in_specs=[VMEM],
        out_specs=VMEM,
        compiler_params=params(),
        cost_estimate=cost(2 * got.size, 4 * got.size),
        name="gathered_sum",
    )(got)


def rotated_cols(basis_t, right):
    dim, narrow = right.shape
    rows = 256

    def body(basis_ref, right_ref, out_ref, low_ref):
        value = product(basis_ref[...], right_ref[...])
        out_ref[...] = value
        low_ref[...] = value.astype(BF16)

    block = pl.BlockSpec((rows, narrow), lambda i: (i, 0))
    return pl.pallas_call(
        body,
        out_shape=[
            jax.ShapeDtypeStruct((dim, narrow), F32),
            jax.ShapeDtypeStruct((dim, narrow), BF16),
        ],
        grid=(dim // rows,),
        in_specs=[
            pl.BlockSpec((rows, dim), lambda i: (i, 0)),
            pl.BlockSpec((dim, narrow), lambda i: (0, 0)),
        ],
        out_specs=[block, block],
        compiler_params=params(),
        cost_estimate=cost(2 * dim * dim * narrow, 2 * dim * dim),
        name="rotated_cols",
    )(basis_t, right)


def undone_copies(rot, back, kernel_t, basis_t, plane, groups, width):
    dim, narrow = rot.shape

    def body(plane_ref, rot_ref, back_ref, kernel_ref, basis_ref, out_ref):
        scaled = (rot_ref[...].T + back_ref[...].astype(F32)) * kernel_ref[...]
        high = scaled.astype(BF16)
        low = (scaled - high.astype(F32)).astype(BF16)
        basis = basis_ref[...]
        value = (product(high, basis) + product(low, basis)).astype(BF16)

        def store(i, carry):
            out_ref[i] = value
            return carry

        lax.fori_loop(0, groups, store, 0)

    full = lambda shape: pl.BlockSpec(shape, lambda i, plane_ref: (0,) * len(shape))
    return pl.pallas_call(
        body,
        out_shape=jax.ShapeDtypeStruct((groups, narrow, width), BF16),
        grid_spec=pltpu.PrefetchScalarGridSpec(
            num_scalar_prefetch=1,
            grid=(1,),
            in_specs=[
                full((dim, narrow)),
                full((narrow, dim)),
                full((narrow, dim)),
                pl.BlockSpec((dim, width), lambda i, plane_ref: (0, plane_ref[0])),
            ],
            out_specs=full((groups, narrow, width)),
        ),
        compiler_params=params(),
        cost_estimate=cost(4 * dim * narrow * width, 4 * dim * width),
        name="undone_copies",
    )(plane, rot, back, kernel_t, basis_t)


def first_product(places, told, whiten, blocks):
    n, width = blocks[0][0].shape
    dim = whiten.shape[0]
    planes = len(blocks)
    rows = 256

    def body(place_ref, told_ref, whiten_ref, *refs):
        centered_ref, out_ref = refs[-2:]
        total = jnp.zeros((rows, width), F32)
        for h in range(planes):
            at = pl.ds(pl.multiple_of(place_ref[h] * width, width), width)
            mean_x, mean_g = told_ref[2 * h : 2 * h + 1, :], told_ref[2 * h + 1 : 2 * h + 2, :]
            shifted = (refs[2 * h][...].astype(F32) - mean_g).astype(BF16)
            total += product(shifted, whiten_ref[at, :])
            centered_ref[:, at] = (refs[2 * h + 1][...].astype(F32) - mean_x).astype(BF16)
        out_ref[...] = total

    full = lambda shape: pl.BlockSpec(shape, lambda i, place_ref: (0,) * len(shape))
    part = lambda cols: pl.BlockSpec((rows, cols), lambda i, place_ref: (i, 0))
    flat = [b for pair in blocks for b in pair]
    return pl.pallas_call(
        body,
        out_shape=[
            jax.ShapeDtypeStruct((n, dim), BF16),
            jax.ShapeDtypeStruct((n, width), F32),
        ],
        grid_spec=pltpu.PrefetchScalarGridSpec(
            num_scalar_prefetch=1,
            grid=(n // rows,),
            in_specs=[full(told.shape), full(whiten.shape)] + [part(width)] * len(flat),
            out_specs=[part(dim), part(width)],
        ),
        compiler_params=params(),
        cost_estimate=cost(2 * n * dim * width, 6 * n * dim),
        name="first_product",
    )(places, told, whiten, *flat)


def last_product(undone, basis_t, centered, running, scale):
    dim, width = undone.shape
    n = centered.shape[0]
    cols = 256

    def body(undone_ref, basis_ref, centered_ref, running_ref, out_ref, turned_ref, total_ref):
        step = pl.program_id(0)

        @pl.when(step == 0)
        def _():
            turned_ref[...] = undone_ref[...].T
            total_ref[...] = running_ref[...]

        sens = (product(turned_ref[...], basis_ref[...]) * scale).astype(BF16)
        total_ref[...] += contract_last(centered_ref[...], sens)

        @pl.when(step == pl.num_programs(0) - 1)
        def _():
            out_ref[...] = total_ref[...].astype(BF16)

    full = lambda shape: pl.BlockSpec(shape, lambda i: (0,) * len(shape))
    return pl.pallas_call(
        body,
        out_shape=jax.ShapeDtypeStruct((n, width), BF16),
        grid=(dim // cols,),
        in_specs=[
            full((dim, width)),
            pl.BlockSpec((dim, cols), lambda i: (0, i)),
            pl.BlockSpec((n, cols), lambda i: (0, i)),
            full((n, width)),
        ],
        out_specs=full((n, width)),
        scratch_shapes=[pltpu.VMEM((width, dim), BF16), pltpu.VMEM((n, width), F32)],
        compiler_params=params(),
        cost_estimate=cost(2 * dim * width * (dim + n), 2 * dim * (dim + n)),
        name="last_product",
    )(undone, basis_t, centered, running)


def local(features, grad_out, eigvecs, eigvals, whiten):
    n, width = features.shape
    groups, planes = lax.axis_size("rows"), lax.axis_size("feat")
    total = n * groups
    dim = width * planes
    narrow = eigvecs.shape[1]
    half = planes // 2
    r, f = lax.axis_index("rows"), lax.axis_index("feat")
    way = jnp.where(r % 2 == 0, -1, 1)

    def pass_on(value, hops=1):
        pairs = [
            (a * planes + b, a * planes + (b + (hops if a % 2 == 0 else -hops)) % planes)
            for a in range(groups)
            for b in range(planes)
        ]
        return lax.ppermute(value, ("rows", "feat"), pairs)

    blocks = [(grad_out, features)]
    for _ in range(1, planes):
        blocks.append(tuple(pass_on(b) for b in blocks[-1]))

    sums = jnp.stack([jnp.sum(a, axis=0, dtype=F32) for a in (features, grad_out)])
    means = jnp.sum(copy_for_each(sums, "rows"), axis=0) / total
    packed = jnp.concatenate(three_parts(means))
    told = [packed, pass_on(packed)]
    told.append(pass_on(packed, 2))
    for _ in range(3, planes):
        told.append(pass_on(told[-1]))
    told = [jnp.sum(t.astype(F32).reshape(3, 2, width), axis=0) for t in told]

    basis_rt = copy_for_each(eigvecs.astype(BF16).T, "feat")
    basis_rt = jnp.swapaxes(basis_rt, 0, 1).reshape(narrow, dim)
    basis_t = lax.all_gather(basis_rt, "rows", axis=0, tiled=True)

    own = jnp.concatenate([features.T, grad_out.T], axis=1)
    mean_cols = means.T
    mixed = gram_first(own, mean_cols, jnp.concatenate(told[:half]), blocks[:half], half)
    mixed = gram_last(mixed, own, mean_cols, told[half], blocks[half], half)

    got = exchange(mixed.reshape(groups, width // groups, -1), "rows")
    copies = gathered_sum(got, width, half)
    gram = exchange(copies, "rows").reshape(width, dim)

    twice = jnp.concatenate([basis_rt, basis_rt], axis=1)
    turned = lax.dynamic_slice_in_dim(twice, f * width, dim, axis=1)
    right = contract_last(gram, turned).astype(BF16)
    right = copy_for_each(right, "feat").reshape(dim, narrow)
    rot, low = rotated_cols(basis_t, right)
    back = exchange(low.reshape(groups, narrow, narrow), "rows")
    back = jnp.swapaxes(back, 0, 1).reshape(narrow, dim)
    first = r * narrow
    kernel_t = divided(lax.dynamic_slice_in_dim(eigvals, first, narrow), eigvals, first)

    copies = undone_copies(rot, back, kernel_t, basis_t, f[None], groups, width)
    undone = exchange(copies, "rows").reshape(dim, width)

    places = ((f + way * jnp.arange(planes, dtype=jnp.int32)) % planes).astype(jnp.int32)
    centered, running = first_product(places, jnp.concatenate(told), whiten, blocks)
    return last_product(undone, basis_t, centered, running, 1.0 / total)


def solution(mesh):
    in_specs = (P("rows", "feat"), P("rows", "feat"), P("feat", "rows"), P(), P(None, "feat"))
    out_specs = P("rows", "feat")
    return jax.shard_map(local, mesh=mesh, in_specs=in_specs, out_specs=out_specs, check_vma=False)
```

```python
import jax
import jax.numpy as jnp
from jax import lax
from jax.experimental import pallas as pl
from jax.experimental.pallas import tpu as pltpu
from jax.sharding import PartitionSpec as P


F32 = jnp.float32
BF16 = jnp.bfloat16
VMEM = pl.BlockSpec(memory_space=pltpu.VMEM)
LIMIT = 60 * 1024 * 1024


def copy_for_each(shard, axis):
    copies = jnp.broadcast_to(shard, (lax.axis_size(axis), *shard.shape))
    return lax.all_to_all(copies, axis, split_axis=0, concat_axis=0, tiled=True)


def exchange(parts, axis):
    return lax.all_to_all(parts, axis, split_axis=0, concat_axis=0, tiled=True)


def contract_last(a, b):
    return lax.dot_general(a, b, (((1,), (1,)), ((), ())), preferred_element_type=F32)


def product(a, b):
    return jnp.dot(a, b, preferred_element_type=F32)


def three_parts(x):
    a = lax.reduce_precision(x, 8, 7)
    b = lax.reduce_precision(x - a, 8, 7)
    c = x - a - b
    return [part.astype(BF16) for part in (a, b, c)]


def divided(lam_row, lam_col, first_row):
    on_diag = (
        (first_row + jnp.arange(lam_row.shape[0], dtype=jnp.int32))[:, None]
        == jnp.arange(lam_col.shape[0], dtype=jnp.int32)[None, :]
    )
    root_row = lam_row ** (-0.5)
    root_col = lam_col ** (-0.5)
    gaps_lam = lam_row[:, None] - lam_col[None, :]
    safe_gap = jnp.where(on_diag, jnp.ones_like(gaps_lam), gaps_lam)
    off_diag = (root_row[:, None] - root_col[None, :]) / safe_gap
    diag_vals = -0.5 * lam_row[:, None] ** (-1.5) + jnp.zeros_like(gaps_lam)
    return jnp.where(on_diag, diag_vals, off_diag)


def cost(flops, nbytes):
    return pl.CostEstimate(flops=flops, bytes_accessed=nbytes, transcendentals=0)


def params():
    return pltpu.CompilerParams(vmem_limit_bytes=LIMIT)


def gram_body(hops, half, own_ref, *refs):
    out_ref = refs[-1]
    width, n = own_ref.shape[0], own_ref.shape[1] // 2
    xt, gt = own_ref[:, :n], own_ref[:, n:]
    sum_x = jnp.sum(xt.astype(F32), axis=1, keepdims=True)
    sum_g = jnp.sum(gt.astype(F32), axis=1, keepdims=True)
    for i, h in enumerate(hops):
        grads, inputs = refs[2 * i][...], refs[2 * i + 1][...]
        value = product(xt, grads)
        value -= sum_x * (jnp.sum(grads.astype(F32), axis=0, keepdims=True) * (1.0 / n))
        if h > 0:
            value += product(gt, inputs)
            value -= sum_g * (jnp.sum(inputs.astype(F32), axis=0, keepdims=True) * (1.0 / n))
        if h == half:
            value = 0.5 * value
        out_ref[:, i * width : (i + 1) * width] = value.astype(BF16)


def gram_first(own, blocks, half):
    width, n = own.shape[0], own.shape[1] // 2
    flat = [b for pair in blocks for b in pair]
    return pl.pallas_call(
        lambda *refs: gram_body(range(half), half, *refs),
        out_shape=jax.ShapeDtypeStruct((width, (half + 1) * width), BF16),
        grid=(1,),
        in_specs=[VMEM] * (1 + len(flat)),
        out_specs=pl.BlockSpec((width, half * width), lambda i: (0, 0)),
        compiler_params=params(),
        cost_estimate=cost(4 * half * n * width * width, 2 * n * width * 2 * (half + 1)),
        name="gram_first",
    )(own, *flat)


def gram_last(partial, own, block, half):
    width, n = own.shape[0], own.shape[1] // 2

    def body(partial_ref, *refs):
        gram_body((half,), half, *refs)

    return pl.pallas_call(
        body,
        out_shape=jax.ShapeDtypeStruct(partial.shape, BF16),
        grid=(1,),
        in_specs=[pl.BlockSpec(memory_space=pl.ANY)] + [VMEM] * 3,
        out_specs=pl.BlockSpec((width, width), lambda i: (0, half)),
        input_output_aliases={0: 0},
        compiler_params=params(),
        cost_estimate=cost(4 * n * width * width, 8 * n * width),
        name="gram_last",
    )(partial, own, *block)


def gathered_sum(got, width, half):
    groups, few, _ = got.shape

    def body(got_ref, out_ref):
        def add(i, sums):
            return sums[0] + got_ref[2 * i].astype(F32), sums[1] + got_ref[2 * i + 1].astype(F32)

        zero = jnp.zeros(got_ref.shape[1:], F32)
        down, up = lax.fori_loop(0, groups // 2, add, (zero, zero))
        piece = lambda a, h: a[:, h * width : (h + 1) * width]
        pair = [piece(down, 0) + piece(up, 0)]
        pair += [piece(up, h) for h in range(1, half)]
        pair += [piece(down, half) + piece(up, half)]
        pair += [piece(down, h) for h in range(half - 1, 0, -1)]
        value = jnp.concatenate(pair, axis=1).astype(BF16)

        def store(i, carry):
            out_ref[i] = value
            return carry

        lax.fori_loop(0, groups, store, 0)

    return pl.pallas_call(
        body,
        out_shape=jax.ShapeDtypeStruct((groups, few, 2 * half * width), BF16),
        in_specs=[VMEM],
        out_specs=VMEM,
        compiler_params=params(),
        cost_estimate=cost(2 * got.size, 4 * got.size),
        name="gathered_sum",
    )(got)


def rotated_cols(basis_t, shared, spread):
    dim, narrow = basis_t.shape[0], spread.shape[0]
    planes, _, width = shared.shape
    rows = 256
    each = rows // narrow

    def body(basis_ref, shared_ref, spread_ref, out_ref, low_ref, right_ref):
        @pl.when(pl.program_id(0) == 0)
        def _():
            for p in range(planes):
                right_ref[:, p * width : (p + 1) * width] = shared_ref[p, :narrow, :]

        value = contract_last(basis_ref[...], right_ref[...])
        out_ref[...] = value
        for k in range(each):
            piece = value[k * narrow : (k + 1) * narrow].astype(BF16)
            low_ref[k] = jnp.concatenate([piece, spread_ref[...]], axis=1)

    return pl.pallas_call(
        body,
        out_shape=[
            jax.ShapeDtypeStruct((dim, narrow), F32),
            jax.ShapeDtypeStruct((dim // narrow, narrow, 2 * narrow), BF16),
        ],
        grid=(dim // rows,),
        in_specs=[
            pl.BlockSpec((rows, dim), lambda i: (i, 0)),
            pl.BlockSpec(shared.shape, lambda i: (0, 0, 0)),
            pl.BlockSpec(spread.shape, lambda i: (0, 0)),
        ],
        out_specs=[
            pl.BlockSpec((rows, narrow), lambda i: (i, 0)),
            pl.BlockSpec((each, narrow, 2 * narrow), lambda i: (i, 0, 0)),
        ],
        scratch_shapes=[pltpu.VMEM((narrow, dim), BF16)],
        compiler_params=params(),
        cost_estimate=cost(2 * dim * dim * narrow, 2 * dim * dim),
        name="rotated_cols",
    )(basis_t, shared, spread)


def undone_copies(rot, back, spread, kernel_t, basis_t, plane, n, width):
    dim, narrow = rot.shape
    groups = back.shape[0]

    def body(plane_ref, rot_ref, back_ref, spread_ref, kernel_ref, basis_ref, out_ref):
        halfway = narrow // 2
        crossed = jnp.concatenate([spread_ref[halfway:, :], spread_ref[:halfway, :]], axis=0)
        crossed = crossed.T.astype(BF16)
        total = jnp.zeros(out_ref.shape[1:], F32)
        for p in range(groups // 2):
            at = slice(2 * p * narrow, 2 * (p + 1) * narrow)
            two = (back_ref[2 * p], back_ref[2 * p + 1])
            mirrored = jnp.concatenate([t[:, :narrow] for t in two], axis=1)
            theirs = jnp.concatenate([t[:, narrow:] for t in two], axis=1)
            scaled = rot_ref[at, :].T + mirrored.astype(F32) + n * product(crossed, theirs)
            scaled = scaled * kernel_ref[:, at]
            high = scaled.astype(BF16)
            low = (scaled - high.astype(F32)).astype(BF16)
            basis = basis_ref[at, :]
            total += product(high, basis) + product(low, basis)
        value = total.astype(BF16)

        def store(i, carry):
            out_ref[i] = value
            return carry

        lax.fori_loop(0, groups, store, 0)

    full = lambda shape: pl.BlockSpec(shape, lambda i, plane_ref: (0,) * len(shape))
    return pl.pallas_call(
        body,
        out_shape=jax.ShapeDtypeStruct((groups, narrow, width), BF16),
        grid_spec=pltpu.PrefetchScalarGridSpec(
            num_scalar_prefetch=1,
            grid=(1,),
            in_specs=[
                full(rot.shape),
                full(back.shape),
                full(spread.shape),
                full(kernel_t.shape),
                pl.BlockSpec((dim, width), lambda i, plane_ref: (0, plane_ref[0])),
            ],
            out_specs=full((groups, narrow, width)),
        ),
        compiler_params=params(),
        cost_estimate=cost(4 * dim * narrow * width, 4 * dim * width),
        name="undone_copies",
    )(plane, rot, back, spread, kernel_t, basis_t)


def first_product(places, told, whiten, blocks):
    n, width = blocks[0][0].shape
    dim = whiten.shape[0]
    planes = len(blocks)
    rows = 256

    def body(place_ref, told_ref, whiten_ref, *refs):
        centered_ref, out_ref = refs[-2:]
        total = jnp.zeros((rows, width), F32)
        for h in range(planes):
            at = pl.ds(pl.multiple_of(place_ref[h] * width, width), width)
            mean_x = told_ref[pl.ds(2 * place_ref[h], 1), :]
            mean_g = told_ref[pl.ds(2 * place_ref[h] + 1, 1), :]
            shifted = (refs[2 * h][...].astype(F32) - mean_g).astype(BF16)
            total += product(shifted, whiten_ref[at, :])
            centered_ref[:, at] = (refs[2 * h + 1][...].astype(F32) - mean_x).astype(BF16)
        out_ref[...] = total

    full = lambda shape: pl.BlockSpec(shape, lambda i, place_ref: (0,) * len(shape))
    part = lambda cols: pl.BlockSpec((rows, cols), lambda i, place_ref: (i, 0))
    flat = [b for pair in blocks for b in pair]
    return pl.pallas_call(
        body,
        out_shape=[
            jax.ShapeDtypeStruct((n, dim), BF16),
            jax.ShapeDtypeStruct((n, width), F32),
        ],
        grid_spec=pltpu.PrefetchScalarGridSpec(
            num_scalar_prefetch=1,
            grid=(n // rows,),
            in_specs=[full(told.shape), full(whiten.shape)] + [part(width)] * len(flat),
            out_specs=[part(dim), part(width)],
        ),
        compiler_params=params(),
        cost_estimate=cost(2 * n * dim * width, 6 * n * dim),
        name="first_product",
    )(places, told, whiten, *flat)


def local(features, grad_out, eigvecs, eigvals, whiten):
    n, width = features.shape
    groups, planes = lax.axis_size("rows"), lax.axis_size("feat")
    total = n * groups
    dim = width * planes
    narrow = eigvecs.shape[1]
    half = planes // 2
    r, f = lax.axis_index("rows"), lax.axis_index("feat")
    way = jnp.where(r % 2 == 0, -1, 1)

    def pass_on(value, hops=1):
        pairs = [
            (a * planes + b, a * planes + (b + (hops if a % 2 == 0 else -hops)) % planes)
            for a in range(groups)
            for b in range(planes)
        ]
        return lax.ppermute(value, ("rows", "feat"), pairs)

    blocks = [(grad_out, features)]
    for _ in range(1, planes):
        blocks.append(tuple(pass_on(b) for b in blocks[-1]))

    sums = jnp.stack([jnp.sum(a, axis=0, dtype=F32) for a in (features, grad_out)])
    all_sums = copy_for_each(sums, "rows")
    means = jnp.sum(all_sums, axis=0) / total
    apart = jnp.swapaxes(all_sums * (1.0 / n) - means, 0, 1).reshape(2 * groups, width)
    spread = jnp.dot(apart, eigvecs, precision=lax.Precision.HIGHEST).astype(BF16)
    few = spread.size // width
    fold = spread.shape[0] // few
    spread = jnp.concatenate([spread[k * few : (k + 1) * few] for k in range(fold)], axis=1)

    basis_rt = copy_for_each(eigvecs.astype(BF16).T, "feat")
    basis_rt = jnp.swapaxes(basis_rt, 0, 1).reshape(narrow, dim)
    basis_t = lax.all_gather(basis_rt, "rows", axis=0, tiled=True)

    own = jnp.concatenate([features.T, grad_out.T], axis=1)
    mixed = gram_first(own, blocks[:half], half)
    mixed = gram_last(mixed, own, blocks[half], half)

    got = exchange(mixed.reshape(groups, width // groups, -1), "rows")
    copies = gathered_sum(got, width, half)
    gram = exchange(copies, "rows").reshape(width, dim)

    twice = jnp.concatenate([basis_rt, basis_rt], axis=1)
    turned = lax.dynamic_slice_in_dim(twice, f * width, dim, axis=1)
    right = contract_last(turned, gram).astype(BF16)
    shared = copy_for_each(jnp.concatenate([right, spread, *three_parts(means)]), "feat")
    spread = jnp.sum(shared[:, narrow : narrow + few].astype(F32), axis=0)
    spread = jnp.concatenate(
        [spread[:, k * narrow : (k + 1) * narrow] for k in range(fold)], axis=0
    )
    rot, low = rotated_cols(basis_t, shared, spread.astype(BF16))
    back = exchange(low, "rows")
    first = r * narrow
    kernel_t = divided(lax.dynamic_slice_in_dim(eigvals, first, narrow), eigvals, first)

    copies = undone_copies(rot, back, spread, kernel_t, basis_t, f[None], float(n), width)
    undone = exchange(copies, "rows").reshape(dim, width)

    places = ((f + way * jnp.arange(planes, dtype=jnp.int32)) % planes).astype(jnp.int32)
    told = shared[:, narrow + few :].astype(F32).reshape(planes, 3, 2, width)
    told = jnp.sum(told, axis=1).reshape(2 * planes, width)
    centered, running = first_product(places, told, whiten, blocks)
    turned = lax.optimization_barrier(contract_last(centered, basis_t).astype(BF16))
    return (running + product(turned, undone) * (1.0 / total)).astype(BF16)


def solution(mesh):
    in_specs = (P("rows", "feat"), P("rows", "feat"), P("feat", "rows"), P(), P(None, "feat"))
    out_specs = P("rows", "feat")
    return jax.shard_map(local, mesh=mesh, in_specs=in_specs, out_specs=out_specs, check_vma=False)
```

```python
import jax
import jax.numpy as jnp
from jax import lax
from jax.experimental import pallas as pl
from jax.experimental.pallas import tpu as pltpu
from jax.sharding import PartitionSpec as P


F32 = jnp.float32
BF16 = jnp.bfloat16
VMEM = pl.BlockSpec(memory_space=pltpu.VMEM)
LIMIT = 60 * 1024 * 1024
SMALL = 20 * 1024 * 1024


def copy_for_each(shard, axis):
    copies = jnp.broadcast_to(shard, (lax.axis_size(axis), *shard.shape))
    return lax.all_to_all(copies, axis, split_axis=0, concat_axis=0, tiled=True)


def exchange(parts, axis):
    return lax.all_to_all(parts, axis, split_axis=0, concat_axis=0, tiled=True)


def contract_last(a, b):
    return lax.dot_general(a, b, (((1,), (1,)), ((), ())), preferred_element_type=F32)


def product(a, b):
    return jnp.dot(a, b, preferred_element_type=F32)


def three_parts(x):
    a = lax.reduce_precision(x, 8, 7)
    b = lax.reduce_precision(x - a, 8, 7)
    c = x - a - b
    return [part.astype(BF16) for part in (a, b, c)]


def divided(lam_row, lam_col, first_row):
    on_diag = (
        (first_row + jnp.arange(lam_row.shape[0], dtype=jnp.int32))[:, None]
        == jnp.arange(lam_col.shape[0], dtype=jnp.int32)[None, :]
    )
    root_row = lam_row ** (-0.5)
    root_col = lam_col ** (-0.5)
    gaps_lam = lam_row[:, None] - lam_col[None, :]
    safe_gap = jnp.where(on_diag, jnp.ones_like(gaps_lam), gaps_lam)
    off_diag = (root_row[:, None] - root_col[None, :]) / safe_gap
    diag_vals = -0.5 * lam_row[:, None] ** (-1.5) + jnp.zeros_like(gaps_lam)
    return jnp.where(on_diag, diag_vals, off_diag)


def cost(flops, nbytes):
    return pl.CostEstimate(flops=flops, bytes_accessed=nbytes, transcendentals=0)


def params(limit=LIMIT):
    return pltpu.CompilerParams(vmem_limit_bytes=limit)


def gram_body(hops, half, own_ref, *refs):
    out_ref = refs[-1]
    width, n = own_ref.shape[0], own_ref.shape[1] // 2
    xt, gt = own_ref[:, :n], own_ref[:, n:]
    sum_x = jnp.sum(xt.astype(F32), axis=1, keepdims=True)
    sum_g = jnp.sum(gt.astype(F32), axis=1, keepdims=True)
    for i, h in enumerate(hops):
        grads, inputs = refs[2 * i][...], refs[2 * i + 1][...]
        value = product(xt, grads)
        value -= sum_x * (jnp.sum(grads.astype(F32), axis=0, keepdims=True) * (1.0 / n))
        if h > 0:
            value += product(gt, inputs)
            value -= sum_g * (jnp.sum(inputs.astype(F32), axis=0, keepdims=True) * (1.0 / n))
        if h == half:
            value = 0.5 * value
        out_ref[:, i * width : (i + 1) * width] = value.astype(BF16)


def gram_first(own, blocks, half):
    width, n = own.shape[0], own.shape[1] // 2
    flat = [b for pair in blocks for b in pair]
    return pl.pallas_call(
        lambda *refs: gram_body(range(half), half, *refs),
        out_shape=jax.ShapeDtypeStruct((width, (half + 1) * width), BF16),
        grid=(1,),
        in_specs=[VMEM] * (1 + len(flat)),
        out_specs=pl.BlockSpec((width, half * width), lambda i: (0, 0)),
        compiler_params=params(),
        cost_estimate=cost(4 * half * n * width * width, 2 * n * width * 2 * (half + 1)),
        name="gram_first",
    )(own, *flat)


def gram_last(partial, own, block, half):
    width, n = own.shape[0], own.shape[1] // 2

    def body(partial_ref, *refs):
        gram_body((half,), half, *refs)

    return pl.pallas_call(
        body,
        out_shape=jax.ShapeDtypeStruct(partial.shape, BF16),
        grid=(1,),
        in_specs=[pl.BlockSpec(memory_space=pl.ANY)] + [VMEM] * 3,
        out_specs=pl.BlockSpec((width, width), lambda i: (0, half)),
        input_output_aliases={0: 0},
        compiler_params=params(),
        cost_estimate=cost(4 * n * width * width, 8 * n * width),
        name="gram_last",
    )(partial, own, *block)


def gathered_sum(got, width, half):
    groups, few, _ = got.shape

    def body(got_ref, out_ref):
        def add(i, sums):
            return sums[0] + got_ref[2 * i].astype(F32), sums[1] + got_ref[2 * i + 1].astype(F32)

        zero = jnp.zeros(got_ref.shape[1:], F32)
        down, up = lax.fori_loop(0, groups // 2, add, (zero, zero))
        piece = lambda a, h: a[:, h * width : (h + 1) * width]
        pair = [piece(down, 0) + piece(up, 0)]
        pair += [piece(up, h) for h in range(1, half)]
        pair += [piece(down, half) + piece(up, half)]
        pair += [piece(down, h) for h in range(half - 1, 0, -1)]
        value = jnp.concatenate(pair, axis=1).astype(BF16)

        def store(i, carry):
            out_ref[i] = value
            return carry

        lax.fori_loop(0, groups, store, 0)

    return pl.pallas_call(
        body,
        out_shape=jax.ShapeDtypeStruct((groups, few, 2 * half * width), BF16),
        in_specs=[VMEM],
        out_specs=VMEM,
        compiler_params=params(SMALL),
        cost_estimate=cost(2 * got.size, 4 * got.size),
        name="gathered_sum",
    )(got)


def rotated_cols(basis_t, shared, spread):
    dim, narrow = basis_t.shape[0], spread.shape[0]
    planes, _, width = shared.shape
    rows = 256
    each = rows // narrow

    def body(basis_ref, shared_ref, spread_ref, out_ref, low_ref, right_ref):
        @pl.when(pl.program_id(0) == 0)
        def _():
            for p in range(planes):
                right_ref[p * width : (p + 1) * width, :] = shared_ref[p, :narrow, :].T

        value = product(basis_ref[...], right_ref[...])
        out_ref[...] = value
        for k in range(each):
            piece = value[k * narrow : (k + 1) * narrow].astype(BF16)
            low_ref[k] = jnp.concatenate([piece, spread_ref[...]], axis=1)

    return pl.pallas_call(
        body,
        out_shape=[
            jax.ShapeDtypeStruct((dim, narrow), F32),
            jax.ShapeDtypeStruct((dim // narrow, narrow, 2 * narrow), BF16),
        ],
        grid=(dim // rows,),
        in_specs=[
            pl.BlockSpec((rows, dim), lambda i: (i, 0)),
            pl.BlockSpec(shared.shape, lambda i: (0, 0, 0)),
            pl.BlockSpec(spread.shape, lambda i: (0, 0)),
        ],
        out_specs=[
            pl.BlockSpec((rows, narrow), lambda i: (i, 0)),
            pl.BlockSpec((each, narrow, 2 * narrow), lambda i: (i, 0, 0)),
        ],
        scratch_shapes=[pltpu.VMEM((dim, narrow), BF16)],
        compiler_params=params(),
        cost_estimate=cost(2 * dim * dim * narrow, 2 * dim * dim),
        name="rotated_cols",
    )(basis_t, shared, spread)


def undone_copies(rot, back, spread, kernel_t, basis, n):
    dim, narrow = rot.shape
    groups, width = back.shape[0], basis.shape[1]

    def body(rot_ref, back_ref, spread_ref, kernel_ref, basis_ref, out_ref):
        halfway = narrow // 2
        crossed = jnp.concatenate([spread_ref[halfway:, :], spread_ref[:halfway, :]], axis=0)
        crossed = crossed.T.astype(BF16)
        total = jnp.zeros(out_ref.shape[1:], F32)
        for p in range(groups // 2):
            at = slice(2 * p * narrow, 2 * (p + 1) * narrow)
            two = (back_ref[2 * p], back_ref[2 * p + 1])
            mirrored = jnp.concatenate([t[:, :narrow] for t in two], axis=1)
            theirs = jnp.concatenate([t[:, narrow:] for t in two], axis=1)
            scaled = rot_ref[at, :].T + mirrored.astype(F32) + n * product(crossed, theirs)
            scaled = scaled * kernel_ref[:, at]
            high = scaled.astype(BF16)
            low = (scaled - high.astype(F32)).astype(BF16)
            total += product(high, basis_ref[at, :]) + product(low, basis_ref[at, :])
        value = total.astype(BF16)

        def store(i, carry):
            out_ref[i] = value
            return carry

        lax.fori_loop(0, groups, store, 0)

    return pl.pallas_call(
        body,
        out_shape=jax.ShapeDtypeStruct((groups, narrow, width), BF16),
        in_specs=[VMEM] * 5,
        out_specs=VMEM,
        compiler_params=params(SMALL),
        cost_estimate=cost(4 * dim * narrow * width, 4 * dim * width),
        name="undone_copies",
    )(rot, back, spread, kernel_t, basis)


def first_product(places, told, whiten, blocks):
    n, width = blocks[0][0].shape
    dim = whiten.shape[0]
    planes = len(blocks)
    rows = 256

    def body(place_ref, told_ref, whiten_ref, *refs):
        centered_ref, out_ref = refs[-2:]
        total = jnp.zeros((rows, width), F32)
        for h in range(planes):
            at = pl.ds(pl.multiple_of(place_ref[h] * width, width), width)
            mean_x = told_ref[pl.ds(2 * place_ref[h], 1), :]
            mean_g = told_ref[pl.ds(2 * place_ref[h] + 1, 1), :]
            shifted = (refs[2 * h][...].astype(F32) - mean_g).astype(BF16)
            total += product(shifted, whiten_ref[at, :])
            centered_ref[:, at] = (refs[2 * h + 1][...].astype(F32) - mean_x).astype(BF16)
        out_ref[...] = total

    full = lambda shape: pl.BlockSpec(shape, lambda i, place_ref: (0,) * len(shape))
    part = lambda cols: pl.BlockSpec((rows, cols), lambda i, place_ref: (i, 0))
    flat = [b for pair in blocks for b in pair]
    return pl.pallas_call(
        body,
        out_shape=[
            jax.ShapeDtypeStruct((n, dim), BF16),
            jax.ShapeDtypeStruct((n, width), F32),
        ],
        grid_spec=pltpu.PrefetchScalarGridSpec(
            num_scalar_prefetch=1,
            grid=(n // rows,),
            in_specs=[full(told.shape), full(whiten.shape)] + [part(width)] * len(flat),
            out_specs=[part(dim), part(width)],
        ),
        compiler_params=params(),
        cost_estimate=cost(2 * n * dim * width, 6 * n * dim),
        name="first_product",
    )(places, told, whiten, *flat)


def local(features, grad_out, eigvecs, eigvals, whiten):
    n, width = features.shape
    groups, planes = lax.axis_size("rows"), lax.axis_size("feat")
    total = n * groups
    dim = width * planes
    narrow = eigvecs.shape[1]
    half = planes // 2
    r, f = lax.axis_index("rows"), lax.axis_index("feat")
    way = jnp.where(r % 2 == 0, -1, 1)

    def pass_on(value, hops=1):
        pairs = [
            (a * planes + b, a * planes + (b + (hops if a % 2 == 0 else -hops)) % planes)
            for a in range(groups)
            for b in range(planes)
        ]
        return lax.ppermute(value, ("rows", "feat"), pairs)

    blocks = [(grad_out, features)]
    for _ in range(1, planes):
        blocks.append(tuple(pass_on(b) for b in blocks[-1]))

    sums = jnp.stack([jnp.sum(a, axis=0, dtype=F32) for a in (features, grad_out)])
    all_sums = copy_for_each(sums, "rows")
    means = jnp.sum(all_sums, axis=0) / total
    apart = jnp.swapaxes(all_sums * (1.0 / n) - means, 0, 1).reshape(2 * groups, width)
    spread = jnp.dot(apart, eigvecs, precision=lax.Precision.HIGHEST).astype(BF16)
    few = spread.size // width
    fold = spread.shape[0] // few
    spread = jnp.concatenate([spread[k * few : (k + 1) * few] for k in range(fold)], axis=1)

    basis_rt = copy_for_each(eigvecs.astype(BF16).T, "feat")
    basis_rt = jnp.swapaxes(basis_rt, 0, 1).reshape(narrow, dim)
    basis_t = lax.all_gather(basis_rt, "rows", axis=0, tiled=True)

    own = jnp.concatenate([features.T, grad_out.T], axis=1)
    mixed = gram_first(own, blocks[:half], half)
    mixed = gram_last(mixed, own, blocks[half], half)

    got = exchange(mixed.reshape(groups, width // groups, -1), "rows")
    copies = gathered_sum(got, width, half)
    gram = exchange(copies, "rows").reshape(width, dim)

    twice = jnp.concatenate([basis_rt, basis_rt], axis=1)
    turned = lax.dynamic_slice_in_dim(twice, f * width, dim, axis=1)
    right = contract_last(turned, gram).astype(BF16)
    shared = copy_for_each(jnp.concatenate([right, spread, *three_parts(means)]), "feat")
    spread = jnp.sum(shared[:, narrow : narrow + few].astype(F32), axis=0)
    spread = jnp.concatenate(
        [spread[:, k * narrow : (k + 1) * narrow] for k in range(fold)], axis=0
    )
    rot, low = rotated_cols(basis_t, shared, spread.astype(BF16))
    back = exchange(low, "rows")
    first = r * narrow
    kernel_t = divided(lax.dynamic_slice_in_dim(eigvals, first, narrow), eigvals, first)

    basis_f = lax.dynamic_slice_in_dim(basis_t, f * width, width, axis=1)
    copies = undone_copies(rot, back, spread, kernel_t, basis_f, float(n))
    undone = exchange(copies, "rows").reshape(dim, width)

    places = ((f + way * jnp.arange(planes, dtype=jnp.int32)) % planes).astype(jnp.int32)
    told = shared[:, narrow + few :].astype(F32).reshape(planes, 3, 2, width)
    told = jnp.sum(told, axis=1).reshape(2 * planes, width)
    centered, running = first_product(places, told, whiten, blocks)
    turned = (contract_last(centered, basis_t) * (1.0 / total)).astype(BF16)
    return (running + product(lax.optimization_barrier(turned), undone)).astype(BF16)


def solution(mesh):
    in_specs = (P("rows", "feat"), P("rows", "feat"), P("feat", "rows"), P(), P(None, "feat"))
    out_specs = P("rows", "feat")
    return jax.shard_map(local, mesh=mesh, in_specs=in_specs, out_specs=out_specs, check_vma=False)
```

```python
import jax
import jax.numpy as jnp
from jax import lax
from jax.experimental import pallas as pl
from jax.experimental.pallas import tpu as pltpu
from jax.sharding import PartitionSpec as P


F32 = jnp.float32
BF16 = jnp.bfloat16
VMEM = pl.BlockSpec(memory_space=pltpu.VMEM)
LIMIT = 60 * 1024 * 1024
SMALL = 20 * 1024 * 1024


def copy_for_each(shard, axis):
    copies = jnp.broadcast_to(shard, (lax.axis_size(axis), *shard.shape))
    return lax.all_to_all(copies, axis, split_axis=0, concat_axis=0, tiled=True)


def exchange(parts, axis):
    return lax.all_to_all(parts, axis, split_axis=0, concat_axis=0, tiled=True)


def contract_last(a, b):
    return lax.dot_general(a, b, (((1,), (1,)), ((), ())), preferred_element_type=F32)


def product(a, b):
    return jnp.dot(a, b, preferred_element_type=F32)


def three_parts(x):
    a = lax.reduce_precision(x, 8, 7)
    b = lax.reduce_precision(x - a, 8, 7)
    c = x - a - b
    return [part.astype(BF16) for part in (a, b, c)]


def divided(lam_row, lam_col, first_row):
    on_diag = (
        (first_row + jnp.arange(lam_row.shape[0], dtype=jnp.int32))[:, None]
        == jnp.arange(lam_col.shape[0], dtype=jnp.int32)[None, :]
    )
    root_row = lam_row ** (-0.5)
    root_col = lam_col ** (-0.5)
    gaps_lam = lam_row[:, None] - lam_col[None, :]
    safe_gap = jnp.where(on_diag, jnp.ones_like(gaps_lam), gaps_lam)
    off_diag = (root_row[:, None] - root_col[None, :]) / safe_gap
    diag_vals = -0.5 * lam_row[:, None] ** (-1.5) + jnp.zeros_like(gaps_lam)
    return jnp.where(on_diag, diag_vals, off_diag)


def cost(flops, nbytes):
    return pl.CostEstimate(flops=flops, bytes_accessed=nbytes, transcendentals=0)


def params(limit=LIMIT):
    return pltpu.CompilerParams(vmem_limit_bytes=limit)


def gram_body(hops, half, own_ref, *refs):
    out_ref = refs[-1]
    width, n = own_ref.shape[0], own_ref.shape[1] // 2
    xt, gt = own_ref[:, :n], own_ref[:, n:]
    sum_x = jnp.sum(xt.astype(F32), axis=1, keepdims=True)
    sum_g = jnp.sum(gt.astype(F32), axis=1, keepdims=True)
    for i, h in enumerate(hops):
        grads, inputs = refs[2 * i][...], refs[2 * i + 1][...]
        value = product(xt, grads)
        value -= sum_x * (jnp.sum(grads.astype(F32), axis=0, keepdims=True) * (1.0 / n))
        if h > 0:
            value += product(gt, inputs)
            value -= sum_g * (jnp.sum(inputs.astype(F32), axis=0, keepdims=True) * (1.0 / n))
        if h == half:
            value = 0.5 * value
        out_ref[:, i * width : (i + 1) * width] = value.astype(BF16)


def gram_first(own, blocks, half):
    width, n = own.shape[0], own.shape[1] // 2
    flat = [b for pair in blocks for b in pair]
    return pl.pallas_call(
        lambda *refs: gram_body(range(half), half, *refs),
        out_shape=jax.ShapeDtypeStruct((width, (half + 1) * width), BF16),
        grid=(1,),
        in_specs=[VMEM] * (1 + len(flat)),
        out_specs=pl.BlockSpec((width, half * width), lambda i: (0, 0)),
        compiler_params=params(),
        cost_estimate=cost(4 * half * n * width * width, 2 * n * width * 2 * (half + 1)),
        name="gram_first",
    )(own, *flat)


def gram_last(partial, own, block, half):
    width, n = own.shape[0], own.shape[1] // 2

    def body(partial_ref, *refs):
        gram_body((half,), half, *refs)

    return pl.pallas_call(
        body,
        out_shape=jax.ShapeDtypeStruct(partial.shape, BF16),
        grid=(1,),
        in_specs=[pl.BlockSpec(memory_space=pl.ANY)] + [VMEM] * 3,
        out_specs=pl.BlockSpec((width, width), lambda i: (0, half)),
        input_output_aliases={0: 0},
        compiler_params=params(),
        cost_estimate=cost(4 * n * width * width, 8 * n * width),
        name="gram_last",
    )(partial, own, *block)


def gathered_sum(got, width, half):
    groups, few, _ = got.shape

    def body(got_ref, out_ref):
        def add(i, sums):
            return sums[0] + got_ref[2 * i].astype(F32), sums[1] + got_ref[2 * i + 1].astype(F32)

        zero = jnp.zeros(got_ref.shape[1:], F32)
        down, up = lax.fori_loop(0, groups // 2, add, (zero, zero))
        piece = lambda a, h: a[:, h * width : (h + 1) * width]
        pair = [piece(down, 0) + piece(up, 0)]
        pair += [piece(up, h) for h in range(1, half)]
        pair += [piece(down, half) + piece(up, half)]
        pair += [piece(down, h) for h in range(half - 1, 0, -1)]
        value = jnp.concatenate(pair, axis=1).astype(BF16)

        def store(i, carry):
            out_ref[i] = value
            return carry

        lax.fori_loop(0, groups, store, 0)

    return pl.pallas_call(
        body,
        out_shape=jax.ShapeDtypeStruct((groups, few, 2 * half * width), BF16),
        in_specs=[VMEM],
        out_specs=VMEM,
        compiler_params=params(SMALL),
        cost_estimate=cost(2 * got.size, 4 * got.size),
        name="gathered_sum",
    )(got)


def rotated_cols(basis_t, shared, spread):
    dim, narrow = basis_t.shape[0], spread.shape[0]
    planes, _, width = shared.shape
    rows = 256
    each = rows // narrow

    def body(basis_ref, shared_ref, spread_ref, out_ref, low_ref, right_ref):
        @pl.when(pl.program_id(0) == 0)
        def _():
            for p in range(planes):
                right_ref[p * width : (p + 1) * width, :] = shared_ref[p, :narrow, :].T

        value = product(basis_ref[...], right_ref[...])
        out_ref[...] = value
        for k in range(each):
            piece = value[k * narrow : (k + 1) * narrow].astype(BF16)
            low_ref[k] = jnp.concatenate([piece, spread_ref[...]], axis=1)

    return pl.pallas_call(
        body,
        out_shape=[
            jax.ShapeDtypeStruct((dim, narrow), F32),
            jax.ShapeDtypeStruct((dim // narrow, narrow, 2 * narrow), BF16),
        ],
        grid=(dim // rows,),
        in_specs=[
            pl.BlockSpec((rows, dim), lambda i: (i, 0)),
            pl.BlockSpec(shared.shape, lambda i: (0, 0, 0)),
            pl.BlockSpec(spread.shape, lambda i: (0, 0)),
        ],
        out_specs=[
            pl.BlockSpec((rows, narrow), lambda i: (i, 0)),
            pl.BlockSpec((each, narrow, 2 * narrow), lambda i: (i, 0, 0)),
        ],
        scratch_shapes=[pltpu.VMEM((dim, narrow), BF16)],
        compiler_params=params(SMALL),
        cost_estimate=cost(2 * dim * dim * narrow, 2 * dim * dim),
        name="rotated_cols",
    )(basis_t, shared, spread)


def undone_copies(rot, back, spread, kernel_t, basis, n):
    dim, narrow = rot.shape
    groups, width = back.shape[0], basis.shape[1]

    def body(rot_ref, back_ref, spread_ref, kernel_ref, basis_ref, out_ref):
        halfway = narrow // 2
        crossed = jnp.concatenate([spread_ref[halfway:, :], spread_ref[:halfway, :]], axis=0)
        crossed = crossed.T.astype(BF16)
        total = jnp.zeros(out_ref.shape[1:], F32)
        for p in range(groups // 2):
            at = slice(2 * p * narrow, 2 * (p + 1) * narrow)
            two = (back_ref[2 * p], back_ref[2 * p + 1])
            mirrored = jnp.concatenate([t[:, :narrow] for t in two], axis=1)
            theirs = jnp.concatenate([t[:, narrow:] for t in two], axis=1)
            scaled = rot_ref[at, :].T + mirrored.astype(F32) + n * product(crossed, theirs)
            scaled = scaled * kernel_ref[:, at]
            high = scaled.astype(BF16)
            low = (scaled - high.astype(F32)).astype(BF16)
            total += product(high, basis_ref[at, :]) + product(low, basis_ref[at, :])
        value = total.astype(BF16)

        def store(i, carry):
            out_ref[i] = value
            return carry

        lax.fori_loop(0, groups, store, 0)

    return pl.pallas_call(
        body,
        out_shape=jax.ShapeDtypeStruct((groups, narrow, width), BF16),
        in_specs=[VMEM] * 5,
        out_specs=VMEM,
        compiler_params=params(SMALL),
        cost_estimate=cost(4 * dim * narrow * width, 4 * dim * width),
        name="undone_copies",
    )(rot, back, spread, kernel_t, basis)


def first_product(places, told, whiten, blocks):
    n, width = blocks[0][0].shape
    dim = whiten.shape[0]
    planes = len(blocks)
    rows = 256

    def body(place_ref, told_ref, whiten_ref, *refs):
        centered_ref, out_ref = refs[-2:]
        total = jnp.zeros((rows, width), F32)
        for h in range(planes):
            at = pl.ds(pl.multiple_of(place_ref[h] * width, width), width)
            mean_x = told_ref[pl.ds(2 * place_ref[h], 1), :]
            mean_g = told_ref[pl.ds(2 * place_ref[h] + 1, 1), :]
            shifted = (refs[2 * h][...].astype(F32) - mean_g).astype(BF16)
            total += product(shifted, whiten_ref[at, :])
            centered_ref[:, at] = (refs[2 * h + 1][...].astype(F32) - mean_x).astype(BF16)
        out_ref[...] = total

    full = lambda shape: pl.BlockSpec(shape, lambda i, place_ref: (0,) * len(shape))
    part = lambda cols: pl.BlockSpec((rows, cols), lambda i, place_ref: (i, 0))
    flat = [b for pair in blocks for b in pair]
    return pl.pallas_call(
        body,
        out_shape=[
            jax.ShapeDtypeStruct((n, dim), BF16),
            jax.ShapeDtypeStruct((n, width), F32),
        ],
        grid_spec=pltpu.PrefetchScalarGridSpec(
            num_scalar_prefetch=1,
            grid=(n // rows,),
            in_specs=[full(told.shape), full(whiten.shape)] + [part(width)] * len(flat),
            out_specs=[part(dim), part(width)],
        ),
        compiler_params=params(SMALL),
        cost_estimate=cost(2 * n * dim * width, 6 * n * dim),
        name="first_product",
    )(places, told, whiten, *flat)


def last_product(turned, undone, running):
    n, dim = turned.shape
    width = undone.shape[1]
    rows = 256

    def body(turned_ref, undone_ref, running_ref, out_ref):
        value = running_ref[...] + product(turned_ref[...], undone_ref[...])
        out_ref[...] = value.astype(BF16)

    part = lambda cols: pl.BlockSpec((rows, cols), lambda i: (i, 0))
    return pl.pallas_call(
        body,
        out_shape=jax.ShapeDtypeStruct((n, width), BF16),
        grid=(n // rows,),
        in_specs=[part(dim), pl.BlockSpec((dim, width), lambda i: (0, 0)), part(width)],
        out_specs=part(width),
        compiler_params=params(SMALL),
        cost_estimate=cost(2 * n * dim * width, 2 * n * dim + 2 * dim * width),
        name="last_product",
    )(turned, undone, running)


def local(features, grad_out, eigvecs, eigvals, whiten):
    n, width = features.shape
    groups, planes = lax.axis_size("rows"), lax.axis_size("feat")
    total = n * groups
    dim = width * planes
    narrow = eigvecs.shape[1]
    half = planes // 2
    r, f = lax.axis_index("rows"), lax.axis_index("feat")
    way = jnp.where(r % 2 == 0, -1, 1)

    def pass_on(value, hops=1):
        pairs = [
            (a * planes + b, a * planes + (b + (hops if a % 2 == 0 else -hops)) % planes)
            for a in range(groups)
            for b in range(planes)
        ]
        return lax.ppermute(value, ("rows", "feat"), pairs)

    blocks = [(grad_out, features)]
    for _ in range(1, planes):
        grads = pass_on(blocks[-1][0])
        blocks.append((grads, pass_on(blocks[-1][1])))

    sums = jnp.stack([jnp.sum(a, axis=0, dtype=F32) for a in (features, grad_out)])
    all_sums = copy_for_each(sums, "rows")
    means = jnp.sum(all_sums, axis=0) / total
    apart = jnp.swapaxes(all_sums * (1.0 / n) - means, 0, 1).reshape(2 * groups, width)
    spread = jnp.dot(apart, eigvecs, precision=lax.Precision.HIGHEST).astype(BF16)
    few = spread.size // width
    fold = spread.shape[0] // few
    spread = jnp.concatenate([spread[k * few : (k + 1) * few] for k in range(fold)], axis=1)

    basis_rt = copy_for_each(eigvecs.astype(BF16).T, "feat")
    basis_rt = jnp.swapaxes(basis_rt, 0, 1).reshape(narrow, dim)
    basis_t = lax.all_gather(basis_rt, "rows", axis=0, tiled=True)

    own = jnp.concatenate([features.T, grad_out.T], axis=1)
    mixed = gram_first(own, blocks[:half], half)
    mixed = gram_last(mixed, own, blocks[half], half)

    got = exchange(mixed.reshape(groups, width // groups, -1), "rows")
    copies = gathered_sum(got, width, half)
    gram = exchange(copies, "rows").reshape(width, dim)

    twice = jnp.concatenate([basis_rt, basis_rt], axis=1)
    turned = lax.dynamic_slice_in_dim(twice, f * width, dim, axis=1)
    right = contract_last(turned, gram).astype(BF16)
    shared = copy_for_each(jnp.concatenate([right, spread, *three_parts(means)]), "feat")
    spread = jnp.sum(shared[:, narrow : narrow + few].astype(F32), axis=0)
    spread = jnp.concatenate(
        [spread[:, k * narrow : (k + 1) * narrow] for k in range(fold)], axis=0
    )
    rot, low = rotated_cols(basis_t, shared, spread.astype(BF16))
    back = exchange(low, "rows")
    first = r * narrow
    kernel_t = divided(lax.dynamic_slice_in_dim(eigvals, first, narrow), eigvals, first)

    basis_f = lax.dynamic_slice_in_dim(basis_t, f * width, width, axis=1)
    copies = undone_copies(rot, back, spread, kernel_t, basis_f, float(n))
    undone = exchange(copies, "rows").reshape(dim, width)

    places = ((f + way * jnp.arange(planes, dtype=jnp.int32)) % planes).astype(jnp.int32)
    told = shared[:, narrow + few :].astype(F32).reshape(planes, 3, 2, width)
    told = jnp.sum(told, axis=1).reshape(2 * planes, width)
    centered, running = first_product(places, told, whiten, blocks)
    turned = (contract_last(centered, basis_t) * (1.0 / total)).astype(BF16)
    return last_product(turned, undone, running)


def solution(mesh):
    in_specs = (P("rows", "feat"), P("rows", "feat"), P("feat", "rows"), P(), P(None, "feat"))
    out_specs = P("rows", "feat")
    return jax.shard_map(local, mesh=mesh, in_specs=in_specs, out_specs=out_specs, check_vma=False)
```

```python
import jax
import jax.numpy as jnp
from jax import lax
from jax.experimental import pallas as pl
from jax.experimental.pallas import tpu as pltpu
from jax.sharding import PartitionSpec as P


F32 = jnp.float32
BF16 = jnp.bfloat16
VMEM = pl.BlockSpec(memory_space=pltpu.VMEM)
LIMIT = 60 * 1024 * 1024
SMALL = 20 * 1024 * 1024


def copy_for_each(shard, axis):
    copies = jnp.broadcast_to(shard, (lax.axis_size(axis), *shard.shape))
    return lax.all_to_all(copies, axis, split_axis=0, concat_axis=0, tiled=True)


def exchange(parts, axis):
    return lax.all_to_all(parts, axis, split_axis=0, concat_axis=0, tiled=True)


def contract_last(a, b):
    return lax.dot_general(a, b, (((1,), (1,)), ((), ())), preferred_element_type=F32)


def product(a, b):
    return jnp.dot(a, b, preferred_element_type=F32)


def three_parts(x):
    a = lax.reduce_precision(x, 8, 7)
    b = lax.reduce_precision(x - a, 8, 7)
    c = x - a - b
    return [part.astype(BF16) for part in (a, b, c)]


def divided(lam_row, lam_col, first_row):
    on_diag = (
        (first_row + jnp.arange(lam_row.shape[0], dtype=jnp.int32))[:, None]
        == jnp.arange(lam_col.shape[0], dtype=jnp.int32)[None, :]
    )
    root_row = lam_row ** (-0.5)
    root_col = lam_col ** (-0.5)
    gaps_lam = lam_row[:, None] - lam_col[None, :]
    safe_gap = jnp.where(on_diag, jnp.ones_like(gaps_lam), gaps_lam)
    off_diag = (root_row[:, None] - root_col[None, :]) / safe_gap
    diag_vals = -0.5 * lam_row[:, None] ** (-1.5) + jnp.zeros_like(gaps_lam)
    return jnp.where(on_diag, diag_vals, off_diag)


def cost(flops, nbytes):
    return pl.CostEstimate(flops=flops, bytes_accessed=nbytes, transcendentals=0)


def params(limit=LIMIT):
    return pltpu.CompilerParams(vmem_limit_bytes=limit)


def gram_body(hops, half, own_ref, *refs):
    out_ref = refs[-1]
    width, n = own_ref.shape[0], own_ref.shape[1] // 2
    xt, gt = own_ref[:, :n], own_ref[:, n:]
    sum_x = jnp.sum(xt.astype(F32), axis=1, keepdims=True)
    sum_g = jnp.sum(gt.astype(F32), axis=1, keepdims=True)
    for i, h in enumerate(hops):
        grads, inputs = refs[2 * i][...], refs[2 * i + 1][...]
        value = product(xt, grads)
        value -= sum_x * (jnp.sum(grads.astype(F32), axis=0, keepdims=True) * (1.0 / n))
        if h > 0:
            value += product(gt, inputs)
            value -= sum_g * (jnp.sum(inputs.astype(F32), axis=0, keepdims=True) * (1.0 / n))
        if h == half:
            value = 0.5 * value
        out_ref[:, i * width : (i + 1) * width] = value.astype(BF16)


def gram_first(own, blocks, half):
    width, n = own.shape[0], own.shape[1] // 2
    flat = [b for pair in blocks for b in pair]
    return pl.pallas_call(
        lambda *refs: gram_body(range(half), half, *refs),
        out_shape=jax.ShapeDtypeStruct((width, (half + 1) * width), BF16),
        grid=(1,),
        in_specs=[VMEM] * (1 + len(flat)),
        out_specs=pl.BlockSpec((width, half * width), lambda i: (0, 0)),
        compiler_params=params(),
        cost_estimate=cost(4 * half * n * width * width, 2 * n * width * 2 * (half + 1)),
        name="gram_first",
    )(own, *flat)


def gram_last(partial, own, block, half):
    width, n = own.shape[0], own.shape[1] // 2

    def body(partial_ref, *refs):
        gram_body((half,), half, *refs)

    return pl.pallas_call(
        body,
        out_shape=jax.ShapeDtypeStruct(partial.shape, BF16),
        grid=(1,),
        in_specs=[pl.BlockSpec(memory_space=pl.ANY)] + [VMEM] * 3,
        out_specs=pl.BlockSpec((width, width), lambda i: (0, half)),
        input_output_aliases={0: 0},
        compiler_params=params(),
        cost_estimate=cost(4 * n * width * width, 8 * n * width),
        name="gram_last",
    )(partial, own, *block)


def gathered_sum(got, width, half):
    groups, few, _ = got.shape

    def body(got_ref, out_ref):
        def add(i, sums):
            return sums[0] + got_ref[2 * i].astype(F32), sums[1] + got_ref[2 * i + 1].astype(F32)

        zero = jnp.zeros(got_ref.shape[1:], F32)
        down, up = lax.fori_loop(0, groups // 2, add, (zero, zero))
        piece = lambda a, h: a[:, h * width : (h + 1) * width]
        pair = [piece(down, 0) + piece(up, 0)]
        pair += [piece(up, h) for h in range(1, half)]
        pair += [piece(down, half) + piece(up, half)]
        pair += [piece(down, h) for h in range(half - 1, 0, -1)]
        value = jnp.concatenate(pair, axis=1).astype(BF16)

        def store(i, carry):
            out_ref[i] = value
            return carry

        lax.fori_loop(0, groups, store, 0)

    return pl.pallas_call(
        body,
        out_shape=jax.ShapeDtypeStruct((groups, few, 2 * half * width), BF16),
        in_specs=[VMEM],
        out_specs=VMEM,
        compiler_params=params(SMALL),
        cost_estimate=cost(2 * got.size, 4 * got.size),
        name="gathered_sum",
    )(got)


def rotated_cols(basis_t, shared, spread):
    dim, narrow = basis_t.shape[0], spread.shape[0]
    planes, _, width = shared.shape
    steps = 8
    rows = dim // steps
    each = rows // narrow

    def body(basis_ref, shared_ref, spread_ref, out_ref, low_ref, held_ref, right_ref, sems):
        copies = [
            pltpu.make_async_copy(
                basis_ref.at[pl.ds(i * rows, rows), :], held_ref.at[i], sems.at[i]
            )
            for i in range(steps)
        ]
        for copy in copies:
            copy.start()
        for p in range(planes):
            right_ref[p * width : (p + 1) * width, :] = shared_ref[p, :narrow, :].T
        for i in range(steps):
            copies[i].wait()
            value = product(held_ref[i], right_ref[...])
            out_ref[i * rows : (i + 1) * rows, :] = value
            for k in range(each):
                piece = value[k * narrow : (k + 1) * narrow].astype(BF16)
                low_ref[i * each + k] = jnp.concatenate([piece, spread_ref[...]], axis=1)

    return pl.pallas_call(
        body,
        out_shape=[
            jax.ShapeDtypeStruct((dim, narrow), F32),
            jax.ShapeDtypeStruct((dim // narrow, narrow, 2 * narrow), BF16),
        ],
        in_specs=[pl.BlockSpec(memory_space=pl.ANY), VMEM, VMEM],
        out_specs=[VMEM, VMEM],
        scratch_shapes=[
            pltpu.VMEM((steps, rows, dim), BF16),
            pltpu.VMEM((dim, narrow), BF16),
            pltpu.SemaphoreType.DMA((steps,)),
        ],
        compiler_params=params(),
        cost_estimate=cost(2 * dim * dim * narrow, 2 * dim * dim),
        name="rotated_cols",
    )(basis_t, shared, spread)


def undone_copies(rot, back, spread, kernel_t, basis, n):
    dim, narrow = rot.shape
    groups, width = back.shape[0], basis.shape[1]

    def body(rot_ref, back_ref, spread_ref, kernel_ref, basis_ref, out_ref):
        halfway = narrow // 2
        crossed = jnp.concatenate([spread_ref[halfway:, :], spread_ref[:halfway, :]], axis=0)
        crossed = crossed.T.astype(BF16)
        total = jnp.zeros(out_ref.shape[1:], F32)
        for p in range(groups // 2):
            at = slice(2 * p * narrow, 2 * (p + 1) * narrow)
            two = (back_ref[2 * p], back_ref[2 * p + 1])
            mirrored = jnp.concatenate([t[:, :narrow] for t in two], axis=1)
            theirs = jnp.concatenate([t[:, narrow:] for t in two], axis=1)
            scaled = rot_ref[at, :].T + mirrored.astype(F32) + n * product(crossed, theirs)
            scaled = scaled * kernel_ref[:, at]
            high = scaled.astype(BF16)
            low = (scaled - high.astype(F32)).astype(BF16)
            total += product(high, basis_ref[at, :]) + product(low, basis_ref[at, :])
        value = total.astype(BF16)

        def store(i, carry):
            out_ref[i] = value
            return carry

        lax.fori_loop(0, groups, store, 0)

    return pl.pallas_call(
        body,
        out_shape=jax.ShapeDtypeStruct((groups, narrow, width), BF16),
        in_specs=[VMEM] * 5,
        out_specs=VMEM,
        compiler_params=params(),
        cost_estimate=cost(4 * dim * narrow * width, 4 * dim * width),
        name="undone_copies",
    )(rot, back, spread, kernel_t, basis)


def first_product(places, told, whiten, blocks):
    n, width = blocks[0][0].shape
    dim = whiten.shape[0]
    planes = len(blocks)
    rows = 256

    def body(place_ref, told_ref, whiten_ref, *refs):
        centered_ref, out_ref = refs[-2:]
        total = jnp.zeros((rows, width), F32)
        for h in range(planes):
            at = pl.ds(pl.multiple_of(place_ref[h] * width, width), width)
            mean_x = told_ref[pl.ds(2 * place_ref[h], 1), :]
            mean_g = told_ref[pl.ds(2 * place_ref[h] + 1, 1), :]
            shifted = (refs[2 * h][...].astype(F32) - mean_g).astype(BF16)
            total += product(shifted, whiten_ref[at, :])
            centered_ref[:, at] = (refs[2 * h + 1][...].astype(F32) - mean_x).astype(BF16)
        out_ref[...] = total

    full = lambda shape: pl.BlockSpec(shape, lambda i, place_ref: (0,) * len(shape))
    part = lambda cols: pl.BlockSpec((rows, cols), lambda i, place_ref: (i, 0))
    flat = [b for pair in blocks for b in pair]
    return pl.pallas_call(
        body,
        out_shape=[
            jax.ShapeDtypeStruct((n, dim), BF16),
            jax.ShapeDtypeStruct((n, width), F32),
        ],
        grid_spec=pltpu.PrefetchScalarGridSpec(
            num_scalar_prefetch=1,
            grid=(n // rows,),
            in_specs=[full(told.shape), full(whiten.shape)] + [part(width)] * len(flat),
            out_specs=[part(dim), part(width)],
        ),
        compiler_params=params(),
        cost_estimate=cost(2 * n * dim * width, 6 * n * dim),
        name="first_product",
    )(places, told, whiten, *flat)


def last_product(turned, undone, running):
    n, dim = turned.shape
    width = undone.shape[1]
    rows = 256

    def body(turned_ref, undone_ref, running_ref, out_ref):
        value = running_ref[...] + product(turned_ref[...], undone_ref[...])
        out_ref[...] = value.astype(BF16)

    part = lambda cols: pl.BlockSpec((rows, cols), lambda i: (i, 0))
    return pl.pallas_call(
        body,
        out_shape=jax.ShapeDtypeStruct((n, width), BF16),
        grid=(n // rows,),
        in_specs=[part(dim), pl.BlockSpec((dim, width), lambda i: (0, 0)), part(width)],
        out_specs=part(width),
        compiler_params=params(),
        cost_estimate=cost(2 * n * dim * width, 2 * n * dim + 2 * dim * width),
        name="last_product",
    )(turned, undone, running)


def local(features, grad_out, eigvecs, eigvals, whiten):
    n, width = features.shape
    groups, planes = lax.axis_size("rows"), lax.axis_size("feat")
    total = n * groups
    dim = width * planes
    narrow = eigvecs.shape[1]
    half = planes // 2
    r, f = lax.axis_index("rows"), lax.axis_index("feat")
    way = jnp.where(r % 2 == 0, -1, 1)

    def pass_on(value, hops=1):
        pairs = [
            (a * planes + b, a * planes + (b + (hops if a % 2 == 0 else -hops)) % planes)
            for a in range(groups)
            for b in range(planes)
        ]
        return lax.ppermute(value, ("rows", "feat"), pairs)

    blocks = [(grad_out, features)]
    for _ in range(1, planes):
        grads = pass_on(blocks[-1][0])
        blocks.append((grads, pass_on(blocks[-1][1])))

    sums = jnp.stack([jnp.sum(a, axis=0, dtype=F32) for a in (features, grad_out)])
    all_sums = copy_for_each(sums, "rows")
    means = jnp.sum(all_sums, axis=0) / total
    apart = jnp.swapaxes(all_sums * (1.0 / n) - means, 0, 1).reshape(2 * groups, width)
    spread = jnp.dot(apart, eigvecs, precision=lax.Precision.HIGHEST).astype(BF16)
    few = spread.size // width
    fold = spread.shape[0] // few
    spread = jnp.concatenate([spread[k * few : (k + 1) * few] for k in range(fold)], axis=1)

    basis_rt = copy_for_each(eigvecs.astype(BF16).T, "feat")
    basis_rt = jnp.swapaxes(basis_rt, 0, 1).reshape(narrow, dim)
    basis_t = lax.all_gather(basis_rt, "rows", axis=0, tiled=True)

    own = jnp.concatenate([features.T, grad_out.T], axis=1)
    mixed = gram_first(own, blocks[:half], half)
    mixed = gram_last(mixed, own, blocks[half], half)

    got = exchange(mixed.reshape(groups, width // groups, -1), "rows")
    copies = gathered_sum(got, width, half)
    gram = exchange(copies, "rows").reshape(width, dim)

    twice = jnp.concatenate([basis_rt, basis_rt], axis=1)
    turned = lax.dynamic_slice_in_dim(twice, f * width, dim, axis=1)
    right = contract_last(turned, gram).astype(BF16)
    shared = copy_for_each(jnp.concatenate([right, spread, *three_parts(means)]), "feat")
    spread = jnp.sum(shared[:, narrow : narrow + few].astype(F32), axis=0)
    spread = jnp.concatenate(
        [spread[:, k * narrow : (k + 1) * narrow] for k in range(fold)], axis=0
    )
    rot, low = rotated_cols(basis_t, shared, spread.astype(BF16))
    back = exchange(low, "rows")
    first = r * narrow
    kernel_t = divided(lax.dynamic_slice_in_dim(eigvals, first, narrow), eigvals, first)

    basis_f = lax.dynamic_slice_in_dim(basis_t, f * width, width, axis=1)
    copies = undone_copies(rot, back, spread, kernel_t, basis_f, float(n))
    undone = exchange(copies, "rows").reshape(dim, width)

    places = ((f + way * jnp.arange(planes, dtype=jnp.int32)) % planes).astype(jnp.int32)
    told = shared[:, narrow + few :].astype(F32).reshape(planes, 3, 2, width)
    told = jnp.sum(told, axis=1).reshape(2 * planes, width)
    centered, running = first_product(places, told, whiten, blocks)
    turned = (contract_last(centered, basis_t) * (1.0 / total)).astype(BF16)
    return last_product(turned, undone, running)


def solution(mesh):
    in_specs = (P("rows", "feat"), P("rows", "feat"), P("feat", "rows"), P(), P(None, "feat"))
    out_specs = P("rows", "feat")
    return jax.shard_map(local, mesh=mesh, in_specs=in_specs, out_specs=out_specs, check_vma=False)
```

```python
import jax
import jax.numpy as jnp
from jax import lax
from jax.experimental import pallas as pl
from jax.experimental.pallas import tpu as pltpu
from jax.sharding import PartitionSpec as P


F32 = jnp.float32
BF16 = jnp.bfloat16
VMEM = pl.BlockSpec(memory_space=pltpu.VMEM)
LIMIT = 60 * 1024 * 1024
SMALL = 20 * 1024 * 1024


def copy_for_each(shard, axis):
    copies = jnp.broadcast_to(shard, (lax.axis_size(axis), *shard.shape))
    return lax.all_to_all(copies, axis, split_axis=0, concat_axis=0, tiled=True)


def exchange(parts, axis):
    return lax.all_to_all(parts, axis, split_axis=0, concat_axis=0, tiled=True)


def contract_last(a, b):
    return lax.dot_general(a, b, (((1,), (1,)), ((), ())), preferred_element_type=F32)


def product(a, b):
    return jnp.dot(a, b, preferred_element_type=F32)


def three_parts(x):
    a = lax.reduce_precision(x, 8, 7)
    b = lax.reduce_precision(x - a, 8, 7)
    c = x - a - b
    return [part.astype(BF16) for part in (a, b, c)]


def divided(lam_row, lam_col, first_row):
    on_diag = (
        (first_row + jnp.arange(lam_row.shape[0], dtype=jnp.int32))[:, None]
        == jnp.arange(lam_col.shape[0], dtype=jnp.int32)[None, :]
    )
    root_row = lam_row ** (-0.5)
    root_col = lam_col ** (-0.5)
    gaps_lam = lam_row[:, None] - lam_col[None, :]
    safe_gap = jnp.where(on_diag, jnp.ones_like(gaps_lam), gaps_lam)
    off_diag = (root_row[:, None] - root_col[None, :]) / safe_gap
    diag_vals = -0.5 * lam_row[:, None] ** (-1.5) + jnp.zeros_like(gaps_lam)
    return jnp.where(on_diag, diag_vals, off_diag)


def cost(flops, nbytes):
    return pl.CostEstimate(flops=flops, bytes_accessed=nbytes, transcendentals=0)


def params(limit=LIMIT):
    return pltpu.CompilerParams(vmem_limit_bytes=limit)


def gram_body(hops, half, own_ref, *refs):
    out_ref = refs[-1]
    width, n = own_ref.shape[0], own_ref.shape[1] // 2
    xt, gt = own_ref[:, :n], own_ref[:, n:]
    sum_x = jnp.sum(xt.astype(F32), axis=1, keepdims=True)
    sum_g = jnp.sum(gt.astype(F32), axis=1, keepdims=True)
    for i, h in enumerate(hops):
        grads, inputs = refs[2 * i][...], refs[2 * i + 1][...]
        value = product(xt, grads)
        value -= sum_x * (jnp.sum(grads.astype(F32), axis=0, keepdims=True) * (1.0 / n))
        if h > 0:
            value += product(gt, inputs)
            value -= sum_g * (jnp.sum(inputs.astype(F32), axis=0, keepdims=True) * (1.0 / n))
        if h == half:
            value = 0.5 * value
        out_ref[:, i * width : (i + 1) * width] = value.astype(BF16)


def gram_first(own, blocks, half):
    width, n = own.shape[0], own.shape[1] // 2
    flat = [b for pair in blocks for b in pair]
    return pl.pallas_call(
        lambda *refs: gram_body(range(half), half, *refs),
        out_shape=jax.ShapeDtypeStruct((width, (half + 1) * width), BF16),
        grid=(1,),
        in_specs=[VMEM] * (1 + len(flat)),
        out_specs=pl.BlockSpec((width, half * width), lambda i: (0, 0)),
        compiler_params=params(),
        cost_estimate=cost(4 * half * n * width * width, 2 * n * width * 2 * (half + 1)),
        name="gram_first",
    )(own, *flat)


def gram_last(partial, own, block, half):
    width, n = own.shape[0], own.shape[1] // 2

    def body(partial_ref, *refs):
        gram_body((half,), half, *refs)

    return pl.pallas_call(
        body,
        out_shape=jax.ShapeDtypeStruct(partial.shape, BF16),
        grid=(1,),
        in_specs=[pl.BlockSpec(memory_space=pl.ANY)] + [VMEM] * 3,
        out_specs=pl.BlockSpec((width, width), lambda i: (0, half)),
        input_output_aliases={0: 0},
        compiler_params=params(),
        cost_estimate=cost(4 * n * width * width, 8 * n * width),
        name="gram_last",
    )(partial, own, *block)


def gathered_sum(got, width, half):
    groups, few, _ = got.shape

    def body(got_ref, out_ref):
        def add(i, sums):
            return sums[0] + got_ref[2 * i].astype(F32), sums[1] + got_ref[2 * i + 1].astype(F32)

        zero = jnp.zeros(got_ref.shape[1:], F32)
        down, up = lax.fori_loop(0, groups // 2, add, (zero, zero))
        piece = lambda a, h: a[:, h * width : (h + 1) * width]
        pair = [piece(down, 0) + piece(up, 0)]
        pair += [piece(up, h) for h in range(1, half)]
        pair += [piece(down, half) + piece(up, half)]
        pair += [piece(down, h) for h in range(half - 1, 0, -1)]
        value = jnp.concatenate(pair, axis=1).astype(BF16)

        def store(i, carry):
            out_ref[2 * i] = value[:, : half * width]
            out_ref[2 * i + 1] = value[:, half * width :]
            return carry

        lax.fori_loop(0, groups // 2, store, 0)

    return pl.pallas_call(
        body,
        out_shape=jax.ShapeDtypeStruct((groups, few, half * width), BF16),
        in_specs=[VMEM],
        out_specs=VMEM,
        compiler_params=params(SMALL),
        cost_estimate=cost(2 * got.size, 4 * got.size),
        name="gathered_sum",
    )(got)


def rotated_cols(basis_t, shared, spread):
    dim, narrow = basis_t.shape[0], spread.shape[0]
    planes, _, width = shared.shape
    steps = 8
    rows = dim // steps
    each = rows // narrow

    def body(basis_ref, shared_ref, spread_ref, out_ref, low_ref, held_ref, right_ref, sems):
        copies = [
            pltpu.make_async_copy(
                basis_ref.at[pl.ds(i * rows, rows), :], held_ref.at[i], sems.at[i]
            )
            for i in range(steps)
        ]
        for copy in copies:
            copy.start()
        for p in range(planes):
            right_ref[p * width : (p + 1) * width, :] = shared_ref[p, :narrow, :].T
        for i in range(steps):
            copies[i].wait()
            value = product(held_ref[i], right_ref[...])
            out_ref[i * rows : (i + 1) * rows, :] = value
            for k in range(each):
                piece = value[k * narrow : (k + 1) * narrow].astype(BF16)
                low_ref[i * each + k] = jnp.concatenate([piece, spread_ref[...]], axis=1)

    return pl.pallas_call(
        body,
        out_shape=[
            jax.ShapeDtypeStruct((dim, narrow), F32),
            jax.ShapeDtypeStruct((dim // narrow, narrow, 2 * narrow), BF16),
        ],
        in_specs=[pl.BlockSpec(memory_space=pl.ANY), VMEM, VMEM],
        out_specs=[VMEM, VMEM],
        scratch_shapes=[
            pltpu.VMEM((steps, rows, dim), BF16),
            pltpu.VMEM((dim, narrow), BF16),
            pltpu.SemaphoreType.DMA((steps,)),
        ],
        compiler_params=params(),
        cost_estimate=cost(2 * dim * dim * narrow, 2 * dim * dim),
        name="rotated_cols",
    )(basis_t, shared, spread)


def undone_copies(rot, back, spread, kernel_t, basis, n):
    dim, narrow = rot.shape
    groups, width = back.shape[0], basis.shape[1]

    def body(*refs):
        out_ref, held, sems = refs[5], refs[6:11], refs[11]
        copies = [pltpu.make_async_copy(refs[k], held[k], sems.at[k]) for k in range(5)]
        for copy in copies:
            copy.start()
        for copy in copies:
            copy.wait()
        rot_ref, back_ref, spread_ref, kernel_ref, basis_ref = held
        halfway = narrow // 2
        crossed = jnp.concatenate([spread_ref[halfway:, :], spread_ref[:halfway, :]], axis=0)
        crossed = crossed.T.astype(BF16)
        total = jnp.zeros(out_ref.shape[1:], F32)
        for p in range(groups // 2):
            at = slice(2 * p * narrow, 2 * (p + 1) * narrow)
            two = (back_ref[2 * p], back_ref[2 * p + 1])
            mirrored = jnp.concatenate([t[:, :narrow] for t in two], axis=1)
            theirs = jnp.concatenate([t[:, narrow:] for t in two], axis=1)
            scaled = rot_ref[at, :].T + mirrored.astype(F32) + n * product(crossed, theirs)
            scaled = scaled * kernel_ref[:, at]
            high = scaled.astype(BF16)
            low = (scaled - high.astype(F32)).astype(BF16)
            total += product(high, basis_ref[at, :]) + product(low, basis_ref[at, :])
        value = total.astype(BF16)

        def store(i, carry):
            out_ref[i] = value
            return carry

        lax.fori_loop(0, groups, store, 0)

    return pl.pallas_call(
        body,
        out_shape=jax.ShapeDtypeStruct((groups, narrow, width), BF16),
        in_specs=[pl.BlockSpec(memory_space=pl.ANY)] * 5,
        out_specs=VMEM,
        scratch_shapes=[pltpu.VMEM(a.shape, a.dtype) for a in (rot, back, spread, kernel_t, basis)]
        + [pltpu.SemaphoreType.DMA((5,))],
        compiler_params=params(),
        cost_estimate=cost(4 * dim * narrow * width, 4 * dim * width),
        name="undone_copies",
    )(rot, back, spread, kernel_t, basis)


def first_product(places, told, whiten, blocks):
    n, width = blocks[0][0].shape
    dim = whiten.shape[0]
    planes = len(blocks)
    rows = 256

    def body(place_ref, told_ref, whiten_ref, *refs):
        centered_ref, out_ref = refs[-2:]
        total = jnp.zeros((rows, width), F32)
        for h in range(planes):
            at = pl.ds(pl.multiple_of(place_ref[h] * width, width), width)
            mean_x = told_ref[pl.ds(2 * place_ref[h], 1), :]
            mean_g = told_ref[pl.ds(2 * place_ref[h] + 1, 1), :]
            shifted = (refs[2 * h][...].astype(F32) - mean_g).astype(BF16)
            total += product(shifted, whiten_ref[at, :])
            centered_ref[:, at] = (refs[2 * h + 1][...].astype(F32) - mean_x).astype(BF16)
        out_ref[...] = total

    full = lambda shape: pl.BlockSpec(shape, lambda i, place_ref: (0,) * len(shape))
    part = lambda cols: pl.BlockSpec((rows, cols), lambda i, place_ref: (i, 0))
    flat = [b for pair in blocks for b in pair]
    return pl.pallas_call(
        body,
        out_shape=[
            jax.ShapeDtypeStruct((n, dim), BF16),
            jax.ShapeDtypeStruct((n, width), F32),
        ],
        grid_spec=pltpu.PrefetchScalarGridSpec(
            num_scalar_prefetch=1,
            grid=(n // rows,),
            in_specs=[full(told.shape), full(whiten.shape)] + [part(width)] * len(flat),
            out_specs=[part(dim), part(width)],
        ),
        compiler_params=params(),
        cost_estimate=cost(2 * n * dim * width, 6 * n * dim),
        name="first_product",
    )(places, told, whiten, *flat)


def last_product(turned, undone, running):
    n, dim = turned.shape
    width = undone.shape[1]
    steps = 4
    rows = n // steps

    def body(turned_ref, undone_ref, running_ref, out_ref, left_ref, right_ref, added_ref, sems):
        first = pltpu.make_async_copy(undone_ref, right_ref, sems.at[steps])
        first.start()
        copies = [
            pltpu.make_async_copy(
                turned_ref.at[pl.ds(i * rows, rows), :], left_ref.at[i], sems.at[i]
            )
            for i in range(steps)
        ]
        for copy in copies:
            copy.start()
        last = pltpu.make_async_copy(running_ref, added_ref, sems.at[steps + 1])
        last.start()
        first.wait()
        last.wait()
        for i in range(steps):
            copies[i].wait()
            at = slice(i * rows, (i + 1) * rows)
            value = added_ref[at, :] + product(left_ref[i], right_ref[...])
            out_ref[at, :] = value.astype(BF16)

    return pl.pallas_call(
        body,
        out_shape=jax.ShapeDtypeStruct((n, width), BF16),
        in_specs=[pl.BlockSpec(memory_space=pl.ANY)] * 3,
        out_specs=VMEM,
        scratch_shapes=[
            pltpu.VMEM((steps, rows, dim), BF16),
            pltpu.VMEM((dim, width), BF16),
            pltpu.VMEM((n, width), F32),
            pltpu.SemaphoreType.DMA((steps + 2,)),
        ],
        compiler_params=params(),
        cost_estimate=cost(2 * n * dim * width, 2 * n * dim + 2 * dim * width),
        name="last_product",
    )(turned, undone, running)


def local(features, grad_out, eigvecs, eigvals, whiten):
    n, width = features.shape
    groups, planes = lax.axis_size("rows"), lax.axis_size("feat")
    total = n * groups
    dim = width * planes
    narrow = eigvecs.shape[1]
    half = planes // 2
    r, f = lax.axis_index("rows"), lax.axis_index("feat")
    way = jnp.where(r % 2 == 0, -1, 1)

    def pass_on(value, hops=1):
        pairs = [
            (a * planes + b, a * planes + (b + (hops if a % 2 == 0 else -hops)) % planes)
            for a in range(groups)
            for b in range(planes)
        ]
        return lax.ppermute(value, ("rows", "feat"), pairs)

    def swap(value):
        pairs = [(a * planes + b, (a ^ 1) * planes + b) for a in range(groups) for b in range(planes)]
        return lax.ppermute(value, ("rows", "feat"), pairs)

    blocks = [(grad_out, features)]
    for _ in range(1, planes):
        grads = pass_on(blocks[-1][0])
        blocks.append((grads, pass_on(blocks[-1][1])))

    sums = jnp.stack([jnp.sum(a, axis=0, dtype=F32) for a in (features, grad_out)])
    all_sums = copy_for_each(sums, "rows")
    means = jnp.sum(all_sums, axis=0) / total
    apart = jnp.swapaxes(all_sums * (1.0 / n) - means, 0, 1).reshape(2 * groups, width)
    spread = jnp.dot(apart, eigvecs, precision=lax.Precision.HIGHEST).astype(BF16)
    few = spread.size // width
    fold = spread.shape[0] // few
    spread = jnp.concatenate([spread[k * few : (k + 1) * few] for k in range(fold)], axis=1)

    basis_rt = copy_for_each(eigvecs.astype(BF16).T, "feat")
    basis_rt = jnp.swapaxes(basis_rt, 0, 1).reshape(narrow, dim)
    both = jnp.concatenate([basis_rt, swap(basis_rt)])
    basis_t = lax.all_gather(basis_rt, "rows", axis=0, tiled=True)

    own = jnp.concatenate([features.T, grad_out.T], axis=1)
    mixed = gram_first(own, blocks[:half], half)
    mixed = gram_last(mixed, own, blocks[half], half)

    got = exchange(mixed.reshape(groups, width // groups, -1), "rows")
    copies = gathered_sum(got, width, half)
    gram = exchange(copies, "rows").reshape(width, half * width)

    twice = jnp.concatenate([both, both], axis=1)
    turned = lax.dynamic_slice_in_dim(twice, f * width + (r % 2) * half * width, half * width, axis=1)
    right = contract_last(turned, gram)
    right = (right[:narrow] + swap(right[narrow:])).astype(BF16)
    shared = copy_for_each(jnp.concatenate([right, spread, *three_parts(means)]), "feat")
    spread = jnp.sum(shared[:, narrow : narrow + few].astype(F32), axis=0)
    spread = jnp.concatenate(
        [spread[:, k * narrow : (k + 1) * narrow] for k in range(fold)], axis=0
    )
    rot, low = rotated_cols(basis_t, shared, spread.astype(BF16))
    back = exchange(low, "rows")
    first = r * narrow
    kernel_t = divided(lax.dynamic_slice_in_dim(eigvals, first, narrow), eigvals, first)

    basis_f = lax.dynamic_slice_in_dim(basis_t, f * width, width, axis=1)
    copies = undone_copies(rot, back, spread, kernel_t, basis_f, float(n))
    undone = exchange(copies, "rows").reshape(dim, width)

    places = ((f + way * jnp.arange(planes, dtype=jnp.int32)) % planes).astype(jnp.int32)
    told = shared[:, narrow + few :].astype(F32).reshape(planes, 3, 2, width)
    told = jnp.sum(told, axis=1).reshape(2 * planes, width)
    centered, running = first_product(places, told, whiten, blocks)
    turned = (contract_last(centered, basis_t) * (1.0 / total)).astype(BF16)
    return last_product(turned, undone, running)


def solution(mesh):
    in_specs = (P("rows", "feat"), P("rows", "feat"), P("feat", "rows"), P(), P(None, "feat"))
    out_specs = P("rows", "feat")
    return jax.shard_map(local, mesh=mesh, in_specs=in_specs, out_specs=out_specs, check_vma=False)
```

```python
import jax
import jax.numpy as jnp
from jax import lax
from jax.experimental import pallas as pl
from jax.experimental.pallas import tpu as pltpu
from jax.sharding import PartitionSpec as P


F32 = jnp.float32
BF16 = jnp.bfloat16
VMEM = pl.BlockSpec(memory_space=pltpu.VMEM)
LIMIT = 60 * 1024 * 1024
SMALL = 20 * 1024 * 1024


def copy_for_each(shard, axis):
    copies = jnp.broadcast_to(shard, (lax.axis_size(axis), *shard.shape))
    return lax.all_to_all(copies, axis, split_axis=0, concat_axis=0, tiled=True)


def exchange(parts, axis):
    return lax.all_to_all(parts, axis, split_axis=0, concat_axis=0, tiled=True)


def contract_last(a, b):
    return lax.dot_general(a, b, (((1,), (1,)), ((), ())), preferred_element_type=F32)


def product(a, b):
    return jnp.dot(a, b, preferred_element_type=F32)


def three_parts(x):
    a = lax.reduce_precision(x, 8, 7)
    b = lax.reduce_precision(x - a, 8, 7)
    c = x - a - b
    return [part.astype(BF16) for part in (a, b, c)]


def divided(lam_row, lam_col, first_row):
    on_diag = (
        (first_row + jnp.arange(lam_row.shape[0], dtype=jnp.int32))[:, None]
        == jnp.arange(lam_col.shape[0], dtype=jnp.int32)[None, :]
    )
    root_row = lam_row ** (-0.5)
    root_col = lam_col ** (-0.5)
    gaps_lam = lam_row[:, None] - lam_col[None, :]
    safe_gap = jnp.where(on_diag, jnp.ones_like(gaps_lam), gaps_lam)
    off_diag = (root_row[:, None] - root_col[None, :]) / safe_gap
    diag_vals = -0.5 * lam_row[:, None] ** (-1.5) + jnp.zeros_like(gaps_lam)
    return jnp.where(on_diag, diag_vals, off_diag)


def cost(flops, nbytes):
    return pl.CostEstimate(flops=flops, bytes_accessed=nbytes, transcendentals=0)


def params(limit=LIMIT):
    return pltpu.CompilerParams(vmem_limit_bytes=limit)


def gram_body(hops, half, own_ref, *refs):
    out_ref = refs[-1]
    width, n = own_ref.shape[0], own_ref.shape[1] // 2
    xt, gt = own_ref[:, :n], own_ref[:, n:]
    sum_x = jnp.sum(xt.astype(F32), axis=1, keepdims=True)
    sum_g = jnp.sum(gt.astype(F32), axis=1, keepdims=True)
    for i, h in enumerate(hops):
        grads, inputs = refs[2 * i][...], refs[2 * i + 1][...]
        value = product(xt, grads)
        value -= sum_x * (jnp.sum(grads.astype(F32), axis=0, keepdims=True) * (1.0 / n))
        if h > 0:
            value += product(gt, inputs)
            value -= sum_g * (jnp.sum(inputs.astype(F32), axis=0, keepdims=True) * (1.0 / n))
        if h == half:
            value = 0.5 * value
        out_ref[:, i * width : (i + 1) * width] = value.astype(BF16)


def gram_first(own, blocks, half):
    width, n = own.shape[0], own.shape[1] // 2
    flat = [b for pair in blocks for b in pair]
    return pl.pallas_call(
        lambda *refs: gram_body(range(half), half, *refs),
        out_shape=jax.ShapeDtypeStruct((width, (half + 1) * width), BF16),
        grid=(1,),
        in_specs=[VMEM] * (1 + len(flat)),
        out_specs=pl.BlockSpec((width, half * width), lambda i: (0, 0)),
        compiler_params=params(),
        cost_estimate=cost(4 * half * n * width * width, 2 * n * width * 2 * (half + 1)),
        name="gram_first",
    )(own, *flat)


def gram_last(partial, own, block, half):
    width, n = own.shape[0], own.shape[1] // 2

    def body(partial_ref, *refs):
        gram_body((half,), half, *refs)

    return pl.pallas_call(
        body,
        out_shape=jax.ShapeDtypeStruct(partial.shape, BF16),
        grid=(1,),
        in_specs=[pl.BlockSpec(memory_space=pl.ANY)] + [VMEM] * 3,
        out_specs=pl.BlockSpec((width, width), lambda i: (0, half)),
        input_output_aliases={0: 0},
        compiler_params=params(),
        cost_estimate=cost(4 * n * width * width, 8 * n * width),
        name="gram_last",
    )(partial, own, *block)


def gathered_sum(got, width, half):
    groups, few, _ = got.shape

    def body(got_ref, out_ref):
        def add(i, sums):
            return sums[0] + got_ref[2 * i].astype(F32), sums[1] + got_ref[2 * i + 1].astype(F32)

        zero = jnp.zeros(got_ref.shape[1:], F32)
        down, up = lax.fori_loop(0, groups // 2, add, (zero, zero))
        piece = lambda a, h: a[:, h * width : (h + 1) * width]
        pair = [piece(down, 0) + piece(up, 0)]
        pair += [piece(up, h) for h in range(1, half)]
        pair += [piece(down, half) + piece(up, half)]
        pair += [piece(down, h) for h in range(half - 1, 0, -1)]
        value = jnp.concatenate(pair, axis=1).astype(BF16)

        def store(i, carry):
            out_ref[2 * i] = value[:, : half * width]
            out_ref[2 * i + 1] = value[:, half * width :]
            return carry

        lax.fori_loop(0, groups // 2, store, 0)

    return pl.pallas_call(
        body,
        out_shape=jax.ShapeDtypeStruct((groups, few, half * width), BF16),
        in_specs=[VMEM],
        out_specs=VMEM,
        compiler_params=params(SMALL),
        cost_estimate=cost(2 * got.size, 4 * got.size),
        name="gathered_sum",
    )(got)


def rotated_cols(basis_t, shared, spread):
    dim, narrow = basis_t.shape[0], spread.shape[0]
    planes, _, width = shared.shape
    steps = 8
    rows = dim // steps
    each = rows // narrow

    def body(basis_ref, shared_ref, spread_ref, out_ref, low_ref, held_ref, right_ref, sems):
        copies = [
            pltpu.make_async_copy(
                basis_ref.at[pl.ds(i * rows, rows), :], held_ref.at[i], sems.at[i]
            )
            for i in range(steps)
        ]
        for copy in copies:
            copy.start()
        for p in range(planes):
            right_ref[p * width : (p + 1) * width, :] = shared_ref[p, :narrow, :].T
        for i in range(steps):
            copies[i].wait()
            value = product(held_ref[i], right_ref[...])
            out_ref[i * rows : (i + 1) * rows, :] = value
            for k in range(each):
                piece = value[k * narrow : (k + 1) * narrow].astype(BF16)
                low_ref[i * each + k] = jnp.concatenate([piece, spread_ref[...]], axis=1)

    return pl.pallas_call(
        body,
        out_shape=[
            jax.ShapeDtypeStruct((dim, narrow), F32),
            jax.ShapeDtypeStruct((dim // narrow, narrow, 2 * narrow), BF16),
        ],
        in_specs=[pl.BlockSpec(memory_space=pl.ANY), VMEM, VMEM],
        out_specs=[VMEM, VMEM],
        scratch_shapes=[
            pltpu.VMEM((steps, rows, dim), BF16),
            pltpu.VMEM((dim, narrow), BF16),
            pltpu.SemaphoreType.DMA((steps,)),
        ],
        compiler_params=params(),
        cost_estimate=cost(2 * dim * dim * narrow, 2 * dim * dim),
        name="rotated_cols",
    )(basis_t, shared, spread)


def undone_copies(rot, back, spread, kernel_t, basis, n):
    dim, narrow = rot.shape
    groups, width = back.shape[0], basis.shape[1]

    def body(rot_ref, back_ref, spread_ref, kernel_ref, basis_ref, out_ref):
        halfway = narrow // 2
        crossed = jnp.concatenate([spread_ref[halfway:, :], spread_ref[:halfway, :]], axis=0)
        crossed = crossed.T.astype(BF16)
        total = jnp.zeros(out_ref.shape[1:], F32)
        for p in range(groups // 2):
            at = slice(2 * p * narrow, 2 * (p + 1) * narrow)
            two = (back_ref[2 * p], back_ref[2 * p + 1])
            mirrored = jnp.concatenate([t[:, :narrow] for t in two], axis=1)
            theirs = jnp.concatenate([t[:, narrow:] for t in two], axis=1)
            scaled = rot_ref[at, :].T + mirrored.astype(F32) + n * product(crossed, theirs)
            scaled = scaled * kernel_ref[:, at]
            high = scaled.astype(BF16)
            low = (scaled - high.astype(F32)).astype(BF16)
            total += product(high, basis_ref[at, :]) + product(low, basis_ref[at, :])
        value = total.astype(BF16)

        def store(i, carry):
            out_ref[i] = value
            return carry

        lax.fori_loop(0, groups, store, 0)

    return pl.pallas_call(
        body,
        out_shape=jax.ShapeDtypeStruct((groups, narrow, width), BF16),
        in_specs=[VMEM] * 5,
        out_specs=VMEM,
        compiler_params=params(SMALL),
        cost_estimate=cost(4 * dim * narrow * width, 4 * dim * width),
        name="undone_copies",
    )(rot, back, spread, kernel_t, basis)


def first_product(places, told, whiten, blocks):
    n, width = blocks[0][0].shape
    dim = whiten.shape[0]
    planes = len(blocks)
    rows = 256

    def body(place_ref, told_ref, whiten_ref, *refs):
        centered_ref, out_ref = refs[-2:]
        total = jnp.zeros((rows, width), F32)
        for h in range(planes):
            at = pl.ds(pl.multiple_of(place_ref[h] * width, width), width)
            mean_x = told_ref[pl.ds(2 * place_ref[h], 1), :]
            mean_g = told_ref[pl.ds(2 * place_ref[h] + 1, 1), :]
            shifted = (refs[2 * h][...].astype(F32) - mean_g).astype(BF16)
            total += product(shifted, whiten_ref[at, :])
            centered_ref[:, at] = (refs[2 * h + 1][...].astype(F32) - mean_x).astype(BF16)
        out_ref[...] = total

    full = lambda shape: pl.BlockSpec(shape, lambda i, place_ref: (0,) * len(shape))
    part = lambda cols: pl.BlockSpec((rows, cols), lambda i, place_ref: (i, 0))
    flat = [b for pair in blocks for b in pair]
    return pl.pallas_call(
        body,
        out_shape=[
            jax.ShapeDtypeStruct((n, dim), BF16),
            jax.ShapeDtypeStruct((n, width), F32),
        ],
        grid_spec=pltpu.PrefetchScalarGridSpec(
            num_scalar_prefetch=1,
            grid=(n // rows,),
            in_specs=[full(told.shape), full(whiten.shape)] + [part(width)] * len(flat),
            out_specs=[part(dim), part(width)],
        ),
        compiler_params=params(),
        cost_estimate=cost(2 * n * dim * width, 6 * n * dim),
        name="first_product",
    )(places, told, whiten, *flat)


def local(features, grad_out, eigvecs, eigvals, whiten):
    n, width = features.shape
    groups, planes = lax.axis_size("rows"), lax.axis_size("feat")
    total = n * groups
    dim = width * planes
    narrow = eigvecs.shape[1]
    half = planes // 2
    r, f = lax.axis_index("rows"), lax.axis_index("feat")
    way = jnp.where(r % 2 == 0, -1, 1)

    def pass_on(value, hops=1):
        pairs = [
            (a * planes + b, a * planes + (b + (hops if a % 2 == 0 else -hops)) % planes)
            for a in range(groups)
            for b in range(planes)
        ]
        return lax.ppermute(value, ("rows", "feat"), pairs)

    def swap(value):
        pairs = [(a * planes + b, (a ^ 1) * planes + b) for a in range(groups) for b in range(planes)]
        return lax.ppermute(value, ("rows", "feat"), pairs)

    blocks = [(grad_out, features)]
    for _ in range(1, planes):
        grads = pass_on(blocks[-1][0])
        blocks.append((grads, pass_on(blocks[-1][1])))

    sums = jnp.stack([jnp.sum(a, axis=0, dtype=F32) for a in (features, grad_out)])
    all_sums = copy_for_each(sums, "rows")
    means = jnp.sum(all_sums, axis=0) / total
    apart = jnp.swapaxes(all_sums * (1.0 / n) - means, 0, 1).reshape(2 * groups, width)
    spread = jnp.dot(apart, eigvecs, precision=lax.Precision.HIGHEST).astype(BF16)
    few = spread.size // width
    fold = spread.shape[0] // few
    spread = jnp.concatenate([spread[k * few : (k + 1) * few] for k in range(fold)], axis=1)

    basis_rt = copy_for_each(eigvecs.astype(BF16).T, "feat")
    basis_rt = jnp.swapaxes(basis_rt, 0, 1).reshape(narrow, dim)
    both = jnp.concatenate([basis_rt, swap(basis_rt)])
    basis_t = lax.all_gather(basis_rt, "rows", axis=0, tiled=True)

    own = jnp.concatenate([features.T, grad_out.T], axis=1)
    mixed = gram_first(own, blocks[:half], half)
    mixed = gram_last(mixed, own, blocks[half], half)

    got = exchange(mixed.reshape(groups, width // groups, -1), "rows")
    copies = gathered_sum(got, width, half)
    gram = exchange(copies, "rows").reshape(width, half * width)

    twice = jnp.concatenate([both, both], axis=1)
    turned = lax.dynamic_slice_in_dim(twice, f * width + (r % 2) * half * width, half * width, axis=1)
    right = contract_last(turned, gram)
    right = (right[:narrow] + swap(right[narrow:])).astype(BF16)
    shared = copy_for_each(jnp.concatenate([right, spread, *three_parts(means)]), "feat")
    spread = jnp.sum(shared[:, narrow : narrow + few].astype(F32), axis=0)
    spread = jnp.concatenate(
        [spread[:, k * narrow : (k + 1) * narrow] for k in range(fold)], axis=0
    )
    rot, low = rotated_cols(basis_t, shared, spread.astype(BF16))
    back = exchange(low, "rows")
    first = r * narrow
    kernel_t = divided(lax.dynamic_slice_in_dim(eigvals, first, narrow), eigvals, first)

    basis_f = lax.dynamic_slice_in_dim(basis_t, f * width, width, axis=1)
    copies = undone_copies(rot, back, spread, kernel_t, basis_f, float(n))
    undone = exchange(copies, "rows").reshape(dim, width)

    places = ((f + way * jnp.arange(planes, dtype=jnp.int32)) % planes).astype(jnp.int32)
    told = shared[:, narrow + few :].astype(F32).reshape(planes, 3, 2, width)
    told = jnp.sum(told, axis=1).reshape(2 * planes, width)
    centered, running = first_product(places, told, whiten, blocks)
    turned = (contract_last(centered, basis_t) * (1.0 / total)).astype(BF16)
    return (running + product(lax.optimization_barrier(turned), undone)).astype(BF16)


def solution(mesh):
    in_specs = (P("rows", "feat"), P("rows", "feat"), P("feat", "rows"), P(), P(None, "feat"))
    out_specs = P("rows", "feat")
    return jax.shard_map(local, mesh=mesh, in_specs=in_specs, out_specs=out_specs, check_vma=False)
```
